32 devices in a mesh: comp: 8 (over z, x), vocab: 4 (over y, core).
Axes of the slice: x: 2, y: 2, z: 4, core: 2. Of those that a mesh axis runs over, the one named last changes fastest.
Arguments:
- hidden: bfloat16 [512, 2048], P('comp'), may hold values from -6 to 6
- routes: int32 [512, 4], P('comp'), may hold values from 0 to 15, all different within a row; in each aligned block of 64 rows (0 to 63, 64 to 127, ...) at most 32 rows name the same one
- targets: int32 [512], P('comp'), may hold values from 0 to 8191
- saved_lse: float32 [512, 4], P('comp'), as said below
- target_logprob: float32 [512, 4], P('comp'), may hold values from -8 to -4
- prior_weight: bfloat16 [2048, 16], P('vocab'), may hold values from -0.25 to 0.25
- projection: bfloat16 [16, 2048, 2048], P('comp', None, 'vocab'), as said below
- embedding: bfloat16 [2048, 8192], P(None, 'vocab'), as said below
Outputs:
- grad_hidden: float32 [512, 2048], P('comp', 'vocab')
- grad_prior: float32 [2048, 16], P('vocab')
- grad_projection: bfloat16 [16, 2048, 2048], P('comp', None, 'vocab')
- grad_embedding: bfloat16 [2048, 8192], P('comp', 'vocab')
The draws below stay inside these ranges and needn't reach their ends.
Inputs may be any that keep to these rules, and one draw needn't show every extreme that they name: `routes`: in each aligned block of 64 rows (the tokens of one index of comp) the 4 entries of a row differ, and no component is named by more than 32 rows; some component reaches 32 in some block. `projection`: entries lie within 4 / sqrt(2048) of zero. `embedding`: entries lie within 6.5 / sqrt(2048) of zero. `saved_lse`: each entry lies between ln(8192) - 2.7 and ln(8192) - 0.9.
All inputs are finite; a program needn't handle non-finite values.
Results may differ from the reference program's by a relative error of at most 0.0056.
Values may be sent and summed in bfloat16 or wider, within the bound.
A program may use at most 128 MiB of HBM per device.

```python
import math
import jax
import jax.numpy as jnp
import numpy as np
from jax import lax

D = 2048
TOP = 4
TOK_DEV = 64
VOCAB = 8192
COMPONENTS = 16
TOKENS = 512
CAP = 32
N_COMP = 8


def draw_hidden(key, part):
    own_key = jax.random.fold_in(key, 12)
    values = jnp.clip(jax.random.normal(own_key, (TOKENS, D), jnp.float32), -6.0, 6.0)
    return values.astype(jnp.bfloat16)


def draw_projection(key, part):
    own_key = jax.random.fold_in(key, 22)
    factor = 1.0 / jnp.sqrt(jnp.float32(D))
    values = jnp.clip(jax.random.normal(own_key, (COMPONENTS, D, D), jnp.float32), -4.0, 4.0) * factor
    return values.astype(jnp.bfloat16)


def draw_embedding(key, part):
    own_key = jax.random.fold_in(key, 31)
    factor = 1.6 / jnp.sqrt(jnp.float32(D))
    values = jnp.clip(jax.random.normal(own_key, (D, VOCAB), jnp.float32), -4.0, 4.0) * factor
    return values.astype(jnp.bfloat16)


def draw_saved_lse(key, part):
    own_key = jax.random.fold_in(key, 41)
    center = jnp.log(jnp.float32(VOCAB)) + 0.5
    offset = jax.random.uniform(own_key, (TOKENS, TOP), jnp.float32, 1.6, 3.0)
    return (center - offset).astype(jnp.float32)


def plant(values, key, smallest, largest):
    longest = values.shape.index(max(values.shape))
    spots = []
    for shift in (0, 1):
        where = [jax.random.randint(jax.random.fold_in(key, axis), (), 0, length) for axis, length in enumerate(values.shape)]
        where[longest] = (where[longest] + shift) % values.shape[longest]
        spots.append(tuple(where))
    return values.at[spots[0]].set(smallest).at[spots[1]].set(largest)


def steps_of(stream_key, shape, pieces, least, top_value):
    def one(dim, parts):
        steps = jax.random.uniform(jax.random.fold_in(jax.random.fold_in(stream_key, 6), dim), (parts,), jnp.float32, least / len(pieces), top_value / len(pieces))
        return jnp.repeat(jnp.exp(steps), shape[dim] // parts).reshape((-1,) + (1,) * (len(shape) - dim - 1))

    gain = one(*pieces[0])
    for cut in pieces[1:]:
        gain = gain * one(*cut)
    return gain


def deal_out(rng, own, number, rows, number_of, top, limit, slope):
    ranking = jax.random.permutation(rng, number_of)
    heavy_load, common = portions_of(number_of, rows * top, limit, slope, True), portions_of(number_of, rows * top, limit, slope, False)
    places = jnp.arange(number_of)

    def named(tallies, rotation):
        used = int((tallies > 0).sum())
        fixed = max(1, used // 4)
        moved = fixed + (places - fixed + rotation * (used - fixed)) % max(1, number_of - fixed)
        return jnp.zeros((number_of,), jnp.int32).at[ranking[jnp.where(places < fixed, places, moved)]].set(jnp.asarray(tallies, jnp.int32))

    tallies = jnp.where(number % 4 == 0, named(heavy_load, number // 4), named(common, number - number // 4 - 1))
    mixed = jax.random.permutation(jax.random.fold_in(own, 3), number_of)
    giver, taker = mixed[0:number_of // 2 * 2:2], mixed[1:number_of // 2 * 2:2]
    margin = jnp.minimum(tallies[giver] - 1, limit - tallies[taker]) // 2
    margin = jnp.where((giver == ranking[0]) | (taker == ranking[0]) | (tallies[taker] == 0), 0, jnp.maximum(margin, 0))
    moved = jax.random.randint(jax.random.fold_in(own, 4), (number_of // 2,), 0, 1 << 20) % (margin + 1)
    tallies = tallies.at[giver].add(-moved).at[taker].add(moved)
    labels = jnp.searchsorted(jnp.cumsum(tallies), jnp.arange(rows * top), side="right").astype(jnp.int32)
    grid = labels.reshape(top, rows).T
    grid = grid[jax.random.permutation(jax.random.fold_in(own, 1), rows)]
    rotation = jax.random.randint(jax.random.fold_in(own, 2), (rows, 1), 0, top)
    return jnp.take_along_axis(grid, (jnp.arange(top)[None, :] + rotation) % top, axis=1)


def portions_of(count, total, bound, lean, full):
    weights = [(1 << 20) // math.isqrt(rank ** lean) + 1 for rank in range(1, count + 1)]
    largest = bound if full else min(bound, max(-(-total // count), total * weights[0] // sum(weights)))
    least = 1 if total - largest >= count - 1 else 0
    holding, surplus = [largest] + [least] * (count - 1), total - largest - least * (count - 1)
    while surplus > 0:
        candidates = [i for i in range(1, count) if holding[i] < largest] or [i for i in range(1, count) if holding[i] < bound]
        pool, left = sum([weights[i] for i in candidates]), surplus
        for i in candidates:
            more = min(bound - holding[i], max(1, left * weights[i] // pool), surplus)
            holding[i] = holding[i] + more
            surplus = surplus - more
    return np.array(holding)


def noise(stream_key, dims, scale, most, split=(), kind=jnp.bfloat16):
    drawn = jax.random.normal(stream_key, dims, jnp.float32) * scale
    if len(split) > 0:
        drawn = steps_of(stream_key, dims, split, -0.22, 0.18) * drawn
    return jnp.clip(drawn, min=-most, max=most).astype(kind)


def setup_inputs(seed: int = 0) -> dict:
    key_list = jax.random.split(jax.random.key(seed), 9)
    hidden = draw_hidden(jax.random.fold_in(key_list[8], 71), 0)
    routes_keys = jax.random.split(jax.random.fold_in(key_list[1], 1), TOKENS // TOK_DEV)
    routes_turns = jax.random.permutation(jax.random.fold_in(key_list[1], 3), TOKENS // TOK_DEV)
    routes = jax.vmap(lambda own, number: deal_out(jax.random.fold_in(key_list[1], 2), own, number, TOK_DEV, COMPONENTS, TOP, CAP, 2))(routes_keys, routes_turns).reshape((TOKENS, TOP))
    targets = plant(jax.random.randint(key_list[2], (TOKENS,), 0, VOCAB), jax.random.fold_in(key_list[2], 1), 0, VOCAB - 1).astype(jnp.int32)
    saved_lse = draw_saved_lse(jax.random.fold_in(key_list[8], 71), 0)
    target_logprob = jnp.clip(-8.0 + 4.0 * jax.random.uniform(key_list[4], (TOKENS, TOP), jnp.float32) ** steps_of(key_list[4], (TOKENS, TOP), ((0, 8),), -0.2, 0.2), -8.0, -4.0)
    prior_weight = noise(key_list[5], (D, COMPONENTS), (D // 4) ** -0.5, 0.25, ((0, 4),))
    projection = draw_projection(jax.random.fold_in(key_list[8], 71), 0)
    embedding = draw_embedding(jax.random.fold_in(key_list[8], 71), 0)
    return {"hidden": hidden, "routes": routes, "targets": targets, "saved_lse": saved_lse, "target_logprob": target_logprob, "prior_weight": prior_weight, "projection": projection, "embedding": embedding}


def reference(hidden, routes, targets, saved_lse, target_logprob, prior_weight, projection, embedding):
    highest = lax.Precision.HIGHEST
    prior_logits = jnp.dot(hidden, prior_weight, preferred_element_type=jnp.float32)
    selected = jnp.take_along_axis(prior_logits, routes, axis=1)
    gate_weights = jax.nn.softmax(selected, axis=-1)
    posterior = jax.nn.softmax(jax.nn.log_softmax(selected, axis=-1) + target_logprob, axis=-1)
    picked = (routes[:, :, None] == jnp.arange(COMPONENTS, dtype=jnp.int32)[None, None, :]).astype(jnp.float32)
    prior_grads = jnp.sum((gate_weights - posterior)[:, :, None] * picked, axis=1)
    grad_prior = jnp.dot(hidden.astype(jnp.float32).T, prior_grads, precision=highest)
    prior_back = jnp.dot(prior_grads, prior_weight.astype(jnp.float32).T, precision=highest)

    slot_rows = N_COMP * CAP
    pair_comp = routes.reshape(N_COMP, TOK_DEV * TOP).astype(jnp.int32)
    pair_onehot = (pair_comp[:, :, None] == jnp.arange(COMPONENTS, dtype=jnp.int32)[None, None, :]).astype(jnp.int32)
    earlier = (jnp.cumsum(pair_onehot, axis=1) - pair_onehot).astype(jnp.int32)
    pair_rank = jnp.sum(earlier * pair_onehot, axis=2).astype(jnp.int32)
    block_ids = jnp.arange(N_COMP, dtype=jnp.int32)[:, None]
    position = (pair_comp * slot_rows + block_ids * CAP + pair_rank).reshape(-1).astype(jnp.int32)
    pair_token = jnp.repeat(jnp.arange(TOKENS, dtype=jnp.int32), TOP)
    slot_total = COMPONENTS * slot_rows
    rows_all = jnp.zeros((slot_total, D), hidden.dtype).at[position].set(hidden[pair_token])
    post_all = jnp.zeros((slot_total,), jnp.float32).at[position].set(posterior.reshape(-1))
    lse_all = jnp.zeros((slot_total,), jnp.float32).at[position].set(saved_lse.reshape(-1))
    target_all = jnp.zeros((slot_total,), jnp.int32).at[position].set(targets[pair_token].astype(jnp.int32))
    vocab_ids = jnp.arange(VOCAB, dtype=jnp.int32)

    def component(running, inputs):
        slot_input, weight, post_rows, lse_rows, target_rows = inputs
        preact = jnp.dot(slot_input, weight, preferred_element_type=jnp.float32)
        tanh_value = jnp.tanh(preact)
        z_rows = tanh_value.astype(jnp.bfloat16)
        logits = jnp.dot(z_rows, embedding, preferred_element_type=jnp.float32)
        target_hit = (target_rows[:, None] == vocab_ids[None, :]).astype(jnp.float32)
        logit_grads = (post_rows[:, None] * (jnp.exp(logits - lse_rows[:, None]) - target_hit)).astype(jnp.bfloat16)
        feature_grads = lax.dot_general(logit_grads, embedding, (((1,), (1,)), ((), ())), preferred_element_type=jnp.float32)
        pre_grads = (feature_grads * (1.0 - tanh_value * tanh_value)).astype(jnp.bfloat16)
        grad_weight = lax.dot_general(slot_input, pre_grads, (((0,), (0,)), ((), ())), preferred_element_type=jnp.float32).astype(jnp.bfloat16)
        slot_grads = lax.dot_general(pre_grads, weight, (((1,), (1,)), ((), ())), preferred_element_type=jnp.float32)
        embed_part = lax.dot_general(z_rows, logit_grads, (((0,), (0,)), ((), ())), preferred_element_type=jnp.float32)
        return running + embed_part, (grad_weight, slot_grads)

    start_sum = jnp.zeros((D, VOCAB), jnp.float32)
    inputs = (rows_all.reshape(COMPONENTS, slot_rows, D), projection, post_all.reshape(COMPONENTS, slot_rows),
              lse_all.reshape(COMPONENTS, slot_rows), target_all.reshape(COMPONENTS, slot_rows))
    embed_sum, (grad_projection, slot_grads) = lax.scan(component, start_sum, inputs)
    pair_grads = slot_grads.reshape(slot_total, D)[position].reshape(TOKENS, TOP, D)
    grad_hidden = jnp.sum(pair_grads, axis=1) + prior_back
    return grad_hidden, grad_prior, grad_projection, embed_sum.astype(jnp.bfloat16)
```

```python
import functools

import jax
import jax.numpy as jnp
from jax import lax
from jax.experimental import pallas as pl
from jax.experimental.pallas import tpu as pltpu
from jax.sharding import PartitionSpec as P

MESH = pl.DeviceIdType.MESH
HIGHEST = lax.Precision.HIGHEST
WORDS = 512


def core_swap(value, count):
    return lax.ppermute(value, "vocab", [(i, i ^ 1) for i in range(count)])


def vocab_gather(block, count):
    me = lax.axis_index("vocab")
    pairs = count // 2
    ring = [(i, (i + 2) % count) for i in range(count)]
    held = [block]
    for _ in range(pairs - 1):
        held.append(lax.ppermute(held[-1], "vocab", ring))
    own = jnp.stack(held)
    other = core_swap(own, count)
    core = me % 2
    both = jnp.where(core == 0, jnp.stack([own, other], 1), jnp.stack([other, own], 1))
    if pairs == 2:
        order = jnp.where(me // 2 == 0, both, both[::-1])
    else:
        order = jnp.take(both, (me // 2 - jnp.arange(pairs)) % pairs, axis=0)
    return order.reshape((count,) + block.shape)


def vocab_scatter(blocks, count, wire):
    me = lax.axis_index("vocab")
    pairs = count // 2
    core, row = me % 2, me // 2
    split = blocks.reshape((pairs, 2) + blocks.shape[1:])
    mine = jnp.where(core == 0, split[:, 0], split[:, 1])
    theirs = jnp.where(core == 0, split[:, 1], split[:, 0])
    mine = mine + core_swap(theirs.astype(wire), count).astype(jnp.float32)
    ring = [(i, (i + 2) % count) for i in range(count)]
    total = lax.dynamic_index_in_dim(mine, (row - 1) % pairs, 0, keepdims=False)
    for step in range(1, pairs):
        got = lax.ppermute(total.astype(wire), "vocab", ring).astype(jnp.float32)
        total = got + lax.dynamic_index_in_dim(mine, (row - 1 - step) % pairs, 0, keepdims=False)
    return total


def comp_scatter(z_rows, grad_rows, owners, wire):
    me = lax.axis_index("comp")
    order = list(range(0, owners, 2)) + list(range(1, owners, 2))[::-1]
    place_of = [order.index(i) for i in range(owners)]
    place = jnp.array(place_of, jnp.int32)[me]
    order_array = jnp.array(order, jnp.int32)
    rows = z_rows.shape[1] // owners
    half = rows // 2

    def part(sign, step):
        owner = order_array[(place - sign * (1 + step)) % owners]
        start = owner * rows + (0 if sign == 1 else half)
        block = lax.dynamic_slice_in_dim(z_rows, start, half, 1)
        return lax.dot_general(
            block, grad_rows, (((0,), (0,)), ((), ())), preferred_element_type=jnp.float32
        )

    totals = []
    rings = [
        (sign, [(order[p], order[(p + sign) % owners]) for p in range(owners)]) for sign in (1, -1)
    ]
    totals = [part(sign, 0) for sign, _ in rings]
    for step in range(1, owners):
        moved = [
            lax.ppermute(total.astype(wire), "comp", ring) for total, (_, ring) in zip(totals, rings)
        ]
        totals = [
            got.astype(jnp.float32) + part(sign, step) for got, (sign, _) in zip(moved, rings)
        ]
    return jnp.concatenate(totals, axis=0)


def shards(hidden, routes, targets, saved_lse, target_logprob, prior_weight, projection, embedding):
    highest = lax.Precision.HIGHEST
    tok_dev, model_width = hidden.shape
    top = routes.shape[1]
    comp_dev = projection.shape[0]
    cols = projection.shape[2]
    voc_dev = embedding.shape[1]
    owners = lax.axis_size("comp")
    slices = lax.axis_size("vocab")
    experts_all = comp_dev * owners
    capacity = max(2, (2 * tok_dev * top + experts_all - 1) // experts_all)
    slot_rows = owners * capacity
    comp_index = lax.axis_index("comp")
    vocab_index = lax.axis_index("vocab")
    wire = jnp.bfloat16 if owners <= 8 else jnp.float32

    own_cols = lax.dynamic_slice_in_dim(hidden, vocab_index * cols, cols, 1)
    cols_all = lax.all_gather(own_cols, "comp", axis=0, tiled=True)
    hidden_all = vocab_gather(cols_all, slices)

    partial_logits = jnp.dot(own_cols, prior_weight, preferred_element_type=jnp.float32)
    prior_logits = lax.psum(partial_logits, "vocab")
    comp_ids = jnp.arange(experts_all, dtype=jnp.int32)
    picked = (routes[:, :, None] == comp_ids[None, None, :]).astype(jnp.float32)
    selected = jnp.sum(picked * prior_logits[:, None, :], axis=2)
    gate = jax.nn.softmax(selected, axis=-1)
    posterior = jax.nn.softmax(jax.nn.log_softmax(selected, axis=-1) + target_logprob, axis=-1)
    prior_grads = jnp.sum((gate - posterior)[:, :, None] * picked, axis=1)
    prior_back = lax.dot_general(
        prior_grads, prior_weight.astype(jnp.float32), (((1,), (1,)), ((), ())), precision=highest
    )
    packed = jnp.concatenate(
        [
            posterior,
            saved_lse,
            jnp.repeat(targets.astype(jnp.float32)[:, None], top, axis=1),
            routes.astype(jnp.float32),
            prior_grads,
        ],
        axis=1,
    )
    packed_all = lax.all_gather(packed, "comp", axis=0, tiled=True)
    grad_prior = lax.dot_general(
        cols_all.astype(jnp.float32),
        packed_all[:, 4 * top :],
        (((0,), (0,)), ((), ())),
        precision=highest,
    )

    pairs = tok_dev * top

    def pair_values(index):
        return packed_all[:, index * top : (index + 1) * top].reshape(owners, pairs)

    pair_comp = pair_values(3)
    own_ids = (comp_index * comp_dev + jnp.arange(comp_dev, dtype=jnp.int32)).astype(jnp.float32)
    hit = pair_comp[None, :, :] == own_ids[:, None, None]
    pair_ids = jnp.arange(pairs, dtype=jnp.int32)
    before = (pair_ids[:, None] < pair_ids[None, :]).astype(jnp.bfloat16)
    rank = jnp.einsum(
        "lbp,pq->lbq", hit.astype(jnp.bfloat16), before, preferred_element_type=jnp.float32
    )
    place = jnp.where(hit, rank, -1.0)
    slot_ids = jnp.arange(capacity, dtype=jnp.int32).astype(jnp.float32)
    dispatch = (place[:, :, None, :] == slot_ids[None, None, :, None]).astype(jnp.float32)

    def to_slots(index):
        values = pair_values(index)
        return jnp.sum(dispatch * values[None, :, None, :], axis=3).reshape(comp_dev * slot_rows)

    post_rows, lse_rows = to_slots(0), to_slots(1)
    target_rows = to_slots(2).astype(jnp.int32)
    fold = (pair_ids[:, None] // top == jnp.arange(tok_dev, dtype=jnp.int32)[None, :]).astype(jnp.bfloat16)
    token_hit = jnp.einsum(
        "lbsp,pt->lbst", dispatch.astype(jnp.bfloat16), fold, preferred_element_type=jnp.float32
    ).astype(jnp.bfloat16)

    rows_in = jnp.einsum(
        "lbst,kbtd->lbskd",
        token_hit,
        hidden_all.reshape(slices, owners, tok_dev, cols),
        preferred_element_type=jnp.float32,
    ).astype(jnp.bfloat16).reshape(comp_dev, slot_rows, model_width)
    preact = jnp.einsum("lrd,lde->lre", rows_in, projection, preferred_element_type=jnp.float32)
    tanh_value = jnp.tanh(preact)
    z_local = tanh_value.astype(jnp.bfloat16).reshape(comp_dev * slot_rows, cols)
    z_blocks = vocab_gather(z_local, slices)
    z_all = jnp.swapaxes(z_blocks, 0, 1).reshape(comp_dev * slot_rows, slices * cols)
    logits = jnp.dot(z_all, embedding, preferred_element_type=jnp.float32)
    vocab_ids = vocab_index * voc_dev + jnp.arange(voc_dev, dtype=jnp.int32)
    target_hit = (target_rows[:, None] == vocab_ids[None, :]).astype(jnp.float32)
    logit_grads = (post_rows[:, None] * (jnp.exp(logits - lse_rows[:, None]) - target_hit)).astype(
        jnp.bfloat16
    )
    logit_grads = lax.optimization_barrier(logit_grads)
    feature_parts = jnp.einsum(
        "rv,kdv->krd",
        logit_grads,
        embedding.reshape(slices, cols, voc_dev),
        preferred_element_type=jnp.float32,
    )
    feature_grads = vocab_scatter(feature_parts, slices, wire).reshape(comp_dev, slot_rows, cols)
    pre_grads = (feature_grads * (1.0 - tanh_value * tanh_value)).astype(jnp.bfloat16)
    slot_parts = jnp.einsum(
        "lre,lkde->klrd",
        pre_grads,
        projection.reshape(comp_dev, slices, model_width // slices, cols),
        preferred_element_type=jnp.float32,
    )
    slot_share = vocab_scatter(slot_parts, slices, wire)
    token_parts = jnp.einsum(
        "lbst,lbsd->btd",
        token_hit.astype(jnp.float32),
        slot_share.reshape(comp_dev, owners, capacity, model_width // slices),
        precision=highest,
    )
    returned = lax.all_to_all(
        token_parts.astype(wire), "comp", split_axis=0, concat_axis=0, tiled=True
    )
    grad_hidden = jnp.sum(returned.astype(jnp.float32), axis=0) + prior_back
    grad_projection = jnp.einsum(
        "lrd,lre->lde", rows_in, pre_grads, preferred_element_type=jnp.float32
    ).astype(jnp.bfloat16)
    grad_embedding = comp_scatter(z_all, logit_grads, owners, wire).astype(jnp.bfloat16)
    return (grad_hidden, grad_prior, grad_projection, grad_embedding)


def capacity_of(owners, hidden, routes, projection):
    tok_dev, top = hidden.shape[0], routes.shape[1]
    experts_all = projection.shape[0] * owners
    return max(2, (2 * tok_dev * top + experts_all - 1) // experts_all)


def fits(owners, slices, hidden, routes, projection, embedding):
    capacity = capacity_of(owners, hidden, routes, projection)
    rows = hidden.shape[1] // owners
    return (
        owners % 2 == 0
        and slices % 2 == 0
        and capacity % 16 == 0
        and (2 * hidden.shape[0]) % 128 == 0
        and rows % 32 == 0
        and embedding.shape[1] % WORDS == 0
        and projection.shape[2] % 128 == 0
    )


def nt_dot(a, b):
    return lax.dot_general(a, b, (((1,), (1,)), ((), ())), preferred_element_type=jnp.float32)


def kernel(
    dims,
    hidden_ref, small_ref, pw_ref, proj_hbm, emb_hbm,
    gh_ref, gprior_ref, ge_ref, xs_ref, pre_ref,
    proj, emb, hid, infoa_out, infoa, infob_out, infob, pwall, dmat, cols3, tl, zall, zt, lacc, lg,
    rbuf, part, facc, fsend, frecv, fysend, fyrecv, sfsend, sfrecv, sfysend, sfyrecv, ss, asend, ain, town, pback,
    load_sem, a_ss, a_rs, b_ss, b_rs, pw_ss, pw_rs, hz_ss, hz_rs, hx_ss, hx_rs, hd_ss, hd_rs,
    zd_ss, zd_rs, zy_ss, zy_rs, zf_ss, zf_rs, r_ss, r_rs, fd_ss, fd_rs, fy_ss, fy_rs, sd_ss, sd_rs, sy_ss, sy_rs,
    t_ss, t_rs,
):
    C, V, L, cap, top, K = dims
    Z, Y = C // 2, V // 2
    T, D = hidden_ref.shape
    cols = pw_ref.shape[1]
    W = emb_hbm.shape[1]
    NS = W // WORDS
    G = L * 2 * cap
    S = Z * G
    half = D // 2
    R2 = D // C
    R = R2 // 2
    T2 = 2 * T
    bf, f32 = jnp.bfloat16, jnp.float32

    c, v = lax.axis_index("comp"), lax.axis_index("vocab")
    z, x = lax.div(c, 2), lax.rem(c, 2)
    y, k = lax.div(v, 2), lax.rem(v, 2)
    xo, ko = 1 - x, 1 - k
    partner = y * 2 + ko

    def zof(i):
        return lax.rem(z + i, Z)

    def zback(i):
        return lax.rem(z + Z - i, Z)

    def yof(i):
        return lax.rem(y + i, Y)

    def yback(i):
        return lax.rem(y + Y - i, Y)

    def rcopy(src, dst, ss_, rs_, **dev):
        return pltpu.make_async_remote_copy(
            src_ref=src, dst_ref=dst, send_sem=ss_, recv_sem=rs_, device_id=dev, device_id_type=MESH
        )

    sends = []

    def send(copy):
        copy.start()
        sends.append(copy)

    load_p = pltpu.make_async_copy(proj_hbm, proj, load_sem.at[0])
    load_e = pltpu.make_async_copy(emb_hbm, emb, load_sem.at[1])
    load_p.start()
    load_e.start()

    comp_peers = [(i, r) for i in range(Z) for r in range(2) if (i, r) != (0, 0)]
    vocab_peers = [(i, r) for i in range(Y) for r in range(2) if (i, r) != (0, 0)]

    def comp_to(i, r):
        return zof(i) * 2 + lax.rem(x + r, 2)

    def comp_from(i, r):
        return zback(i) * 2 + lax.rem(x + r, 2)

    def vocab_to(i, r):
        return yof(i) * 2 + lax.rem(k + r, 2)

    def vocab_from(i, r):
        return yback(i) * 2 + lax.rem(k + r, 2)

    barrier = pltpu.get_barrier_semaphore()
    for i, r in comp_peers:
        pl.semaphore_signal(barrier, inc=1, device_id={"comp": comp_to(i, r)}, device_id_type=MESH)
    for i, r in vocab_peers:
        pl.semaphore_signal(barrier, inc=1, device_id={"vocab": vocab_to(i, r)}, device_id_type=MESH)

    lane = lax.broadcasted_iota(jnp.int32, (K, T2), 1)
    mine = (lane >= x * T) & (lane < x * T + T)
    comp_id = lax.broadcasted_iota(jnp.int32, (K, T2), 0).astype(f32)
    hit = jnp.zeros((K, T2), f32)
    lse_k = jnp.zeros((K, T2), f32)
    tlp_k = jnp.zeros((K, T2), f32)
    for j in range(top):
        named = (small_ref[j : j + 1, :] == comp_id) & mine
        hit = jnp.where(named, 1.0, hit)
        lse_k = jnp.where(named, small_ref[top + j : top + j + 1, :], lse_k)
        tlp_k = jnp.where(named, small_ref[2 * top + j : 2 * top + j + 1, :], tlp_k)
    on = hit > 0.5
    upper = (
        lax.broadcasted_iota(jnp.int32, (T2, T2), 0) < lax.broadcasted_iota(jnp.int32, (T2, T2), 1)
    ).astype(f32).astype(bf)
    rank = jnp.dot(hit.astype(bf), upper, preferred_element_type=f32)
    place = jnp.where(on, rank, -1.0)
    infoa_out[...] = place
    hid[z, pl.ds(pl.multiple_of(x * T, T), T), :] = hidden_ref[...]
    pwall[v] = pw_ref[...]
    pl.semaphore_wait(barrier, len(comp_peers) + len(vocab_peers))

    xrow = pl.ds(pl.multiple_of(x * T, T), T)
    xorow = pl.ds(pl.multiple_of(xo * T, T), T)
    kcol = pl.ds(pl.multiple_of(k * half, half), half)
    kocol = pl.ds(pl.multiple_of(ko * half, half), half)
    send(rcopy(hidden_ref.at[:, kcol], hid.at[z, xrow, kcol], hx_ss.at[0], hx_rs.at[0], comp=z * 2 + xo))
    for i in range(1, Z):
        send(rcopy(hidden_ref.at[:, kcol], hid.at[z, xrow, kcol], hz_ss.at[i], hz_rs.at[i], comp=zof(i) * 2 + x))
    for i, r in vocab_peers:
        n = i * 2 + r
        send(rcopy(pw_ref, pwall.at[v], pw_ss.at[n], pw_rs.at[n], vocab=vocab_to(i, r)))
    for i, r in comp_peers:
        n = i * 2 + r
        send(rcopy(infoa_out, infoa.at[c], a_ss.at[n], a_rs.at[n], comp=comp_to(i, r)))
    infoa[c] = place

    for i, r in vocab_peers:
        n = i * 2 + r
        rcopy(pw_ref, pwall.at[vocab_from(i, r)], pw_ss.at[n], pw_rs.at[n], vocab=vocab_from(i, r)).wait_recv()
    logit = jnp.zeros((K, T), f32)
    for vv in range(V):
        logit = logit + nt_dot(pwall[vv], hidden_ref[:, vv * cols : (vv + 1) * cols])
    logit = jnp.concatenate([logit, logit], axis=1)

    def top_of(values):
        return jnp.max(jnp.where(on, values, -1e30), axis=0, keepdims=True)

    def norm(values):
        total = jnp.sum(values, axis=0, keepdims=True)
        return jnp.where(total > 0.0, total, 1.0)

    shifted = logit - top_of(logit)
    weight = jnp.where(on, jnp.exp(jnp.where(on, shifted, 0.0)), 0.0)
    total = norm(weight)
    gate = weight / total
    mixed = shifted - jnp.log(total) + tlp_k
    mixed = jnp.where(on, mixed - top_of(mixed), 0.0)
    weight = jnp.where(on, jnp.exp(mixed), 0.0)
    post = weight / norm(weight)
    pgrad = gate - post
    target = jnp.where(mine[0:8], jnp.broadcast_to(small_ref[3 * top : 3 * top + 1, :], (8, T2)), 0.0)
    infob_value = jnp.concatenate([post, lse_k, pgrad, target], axis=0)
    infob_out[...] = infob_value
    infob[c] = infob_value
    for i, r in comp_peers:
        n = i * 2 + r
        send(rcopy(infob_out, infob.at[c], b_ss.at[n], b_rs.at[n], comp=comp_to(i, r)))
    pback[...] = lax.dot_general(
        pgrad, pw_ref[...].astype(f32), (((0,), (0,)), ((), ())), precision=HIGHEST, preferred_element_type=f32
    )

    for i, r in comp_peers:
        n = i * 2 + r
        rcopy(infoa_out, infoa.at[comp_from(i, r)], a_ss.at[n], a_rs.at[n], comp=comp_from(i, r)).wait_recv()
    slot_id = lax.broadcasted_iota(jnp.int32, (cap, T2), 0).astype(f32)
    for zz in range(Z):
        for l in range(L):
            for xx in range(2):
                row = infoa[zz * 2 + xx, pl.ds(c * L + l, 1), :]
                start = l * 2 * cap + xx * cap
                dmat[zz, start : start + cap, :] = (row == slot_id).astype(f32).astype(bf)

    def forward(i):
        if i > 0:
            rcopy(hidden_ref.at[:, kcol], hid.at[zback(i), xrow, kcol], hz_ss.at[i], hz_rs.at[i], comp=c).wait_recv()
            piece = hid.at[zback(i), xrow, kcol]
            send(rcopy(piece, piece, hx_ss.at[i], hx_rs.at[i], comp=z * 2 + xo))
            send(rcopy(piece, piece, hd_ss.at[i, 0], hd_rs.at[i, 0], vocab=partner))

    def forward_x(i):
        piece = hid.at[zback(i), xorow, kcol]
        rcopy(piece, piece, hx_ss.at[i], hx_rs.at[i], comp=z * 2 + xo).wait_recv()
        send(rcopy(piece, piece, hd_ss.at[i, 1], hd_rs.at[i, 1], vocab=partner))

    def arrive(i):
        if i > 0:
            piece = hid.at[zback(i), xrow, kocol]
            rcopy(piece, piece, hd_ss.at[i, 0], hd_rs.at[i, 0], vocab=partner).wait_recv()
        piece = hid.at[zback(i), xorow, kocol]
        rcopy(piece, piece, hd_ss.at[i, 1], hd_rs.at[i, 1], vocab=partner).wait_recv()

    def project(i):
        zz = zback(i)
        rows = jnp.dot(dmat[zz], hid[zz], preferred_element_type=f32).astype(bf)
        xs_ref[zz] = rows
        for l in range(L):
            span = slice(l * 2 * cap, (l + 1) * 2 * cap)
            value = jnp.tanh(jnp.dot(rows[span], proj[l], preferred_element_type=f32))
            tl[zz, span, :] = value
            zall[v, zz, span, :] = value.astype(bf)
        piece = zall.at[v, zz]
        for dy in range(1, Y):
            send(rcopy(piece, piece, zy_ss.at[dy, i], zy_rs.at[dy, i], vocab=yof(dy) * 2 + k))
        send(rcopy(piece, piece, zd_ss.at[i], zd_rs.at[i], vocab=partner))

    forward_x(0)
    if Z > 1:
        forward(1)
    load_p.wait()
    arrive(0)
    project(0)
    for i in range(1, Z):
        forward_x(i)
        if i + 1 < Z:
            forward(i + 1)
        arrive(i)
        project(i)
    load_e.wait()

    for i, r in comp_peers:
        n = i * 2 + r
        rcopy(infob_out, infob.at[comp_from(i, r)], b_ss.at[n], b_rs.at[n], comp=comp_from(i, r)).wait_recv()
    for zz in range(Z):
        for l in range(L):
            for xx in range(2):
                b = zz * 2 + xx
                start = l * 2 * cap + xx * cap
                pick = dmat[zz, start : start + cap, :].astype(f32)
                rows3 = (
                    infob[b, pl.ds(c * L + l, 1), :],
                    infob[b, pl.ds(K + c * L + l, 1), :],
                    infob[b, 3 * K : 3 * K + 1, :],
                )
                for q in range(3):
                    cols3[q, zz, start : start + cap, :] = jnp.sum(pick * rows3[q], axis=1, keepdims=True)
    owncols = pl.ds(pl.multiple_of(v * cols, cols), cols)
    gp = jnp.zeros((K, cols), f32)
    for zz in range(Z):
        grads = infob[zz * 2, 2 * K : 3 * K, :] + infob[zz * 2 + 1, 2 * K : 3 * K, :]
        gp = gp + jnp.dot(grads, hid[zz, :, owncols].astype(f32), precision=HIGHEST, preferred_element_type=f32)
    gprior_ref[...] = gp

    def features(vv):
        return zall[vv].reshape(S, cols)

    def feature_rows(vv):
        return pl.ds(pl.multiple_of(vv * cols, cols), cols)

    def zdone(i):
        piece = zall.at[partner, zback(i)]
        rcopy(piece, piece, zd_ss.at[i], zd_rs.at[i], vocab=partner).wait_recv()

    for i in range(Z):
        zdone(i)
        for dy in range(1, Y):
            piece = zall.at[yback(dy) * 2 + k, zback(i)]
            if i < Z - 1:
                rcopy(piece, piece, zy_ss.at[dy, i], zy_rs.at[dy, i], vocab=v).wait_recv()
                send(rcopy(piece, piece, zf_ss.at[dy, i], zf_rs.at[dy, i], vocab=partner))

    def early(j, carry):
        at = pl.ds(pl.multiple_of(j * WORDS, WORDS), WORDS)
        lacc[j] = jnp.dot(
            features(v), emb[feature_rows(v), at], preferred_element_type=f32
        ) + jnp.dot(features(partner), emb[feature_rows(partner), at], preferred_element_type=f32)
        return carry

    lax.fori_loop(0, NS, early, 0)
    for dy in range(1, Y):
        i = Z - 1
        piece = zall.at[yback(dy) * 2 + k, zback(i)]
        rcopy(piece, piece, zy_ss.at[dy, i], zy_rs.at[dy, i], vocab=v).wait_recv()
        send(rcopy(piece, piece, zf_ss.at[dy, i], zf_rs.at[dy, i], vocab=partner))
    for dy in range(1, Y):
        for i in range(Z):
            piece = zall.at[yback(dy) * 2 + ko, zback(i)]
            rcopy(piece, piece, zf_ss.at[dy, i], zf_rs.at[dy, i], vocab=partner).wait_recv()
    for vv in range(V):
        zt[vv * cols : (vv + 1) * cols, :] = features(vv).T

    spot = (1 - x) * z + x * (C - 1 - z)

    def at_spot(p):
        p = lax.rem(p + 2 * C, C)
        high = lax.div(p, Z)
        return (1 - high) * (2 * p) + high * (2 * (C - 1 - p) + 1)

    following = [at_spot(spot + 1), at_spot(spot - 1)]

    def partial(way, s, j):
        sign = 1 if way == 0 else -1
        owner = at_spot(spot - sign * (1 + s))
        rows = pl.ds(pl.multiple_of(owner * R2 + way * R, R), R)
        return jnp.dot(zt[rows, :], lg[j], preferred_element_type=f32)

    def ring_copy(way, s, j):
        return rcopy(
            rbuf.at[way, s, j], rbuf.at[way, s + 1, j], r_ss.at[way, s + 1, j], r_rs.at[way, s + 1, j],
            comp=following[way],
        )

    lse_rows = cols3[1].reshape(S, 1)
    post_rows = cols3[0].reshape(S, 1)
    target_rows = cols3[2].reshape(S, 1).astype(jnp.int32)

    def words(j, carry):
        at = pl.ds(pl.multiple_of(j * WORDS, WORDS), WORDS)
        logits = lacc[j]
        for dy in range(1, Y):
            for kk in range(2):
                vv = yof(dy) * 2 + kk
                logits = logits + jnp.dot(features(vv), emb[feature_rows(vv), at], preferred_element_type=f32)
        ids = v * W + j * WORDS + lax.broadcasted_iota(jnp.int32, (S, WORDS), 1)
        onehot = (target_rows == ids).astype(f32)
        lg[j] = (post_rows * (jnp.exp(logits - lse_rows) - onehot)).astype(bf)
        for way in range(2):
            rbuf[way, 0, j] = partial(way, 0, j).astype(bf)
            ring_copy(way, 0, j).start()
        return carry

    lax.fori_loop(0, NS, words, 0)

    def turn(q, carry):
        s, j = lax.div(q, NS) + 1, lax.rem(q, NS)
        for way in range(2):
            part[way] = partial(way, s, j)
        for way in range(2):
            ring_copy(way, s - 1, j).wait_recv()
            rbuf[way, s, j] = (rbuf[way, s, j].astype(f32) + part[way]).astype(bf)
            ring_copy(way, s, j).start()
        return carry

    turns = [0]

    def ring(count):
        end = min(turns[0] + count, (C - 2) * NS)
        if end > turns[0]:
            lax.fori_loop(turns[0], end, turn, 0)
        turns[0] = end

    def flat(ref):
        return ref[...].reshape(S, cols)

    def feature_part(vv):
        facc[...] = jnp.zeros((S, cols), f32)

        def add(j, carry):
            at = pl.ds(pl.multiple_of(j * WORDS, WORDS), WORDS)
            facc[...] += nt_dot(lg[j], emb[feature_rows(vv), at])
            return carry

        lax.fori_loop(0, NS, add, 0)
        return facc[...]

    def slot_part(vv):
        for l in range(L):
            span = slice(l * 2 * cap, (l + 1) * 2 * cap)
            rows = pre_ref[:, span, :].reshape(Z * 2 * cap, cols)
            value = nt_dot(rows, proj[l, feature_rows(vv), :])
            ss[:, span, :] = value.reshape(Z, 2 * cap, cols)
        return flat(ss)

    def reduce_over(make, out, dsend, drecv, ysend, yrecv, d_ss, d_rs, y_ss, y_rs):
        def swap(i):
            return rcopy(dsend.at[i], drecv.at[i], d_ss.at[i], d_rs.at[i], vocab=partner)

        def give(dy):
            dsend[dy] = make(yof(dy) * 2 + ko).astype(bf)
            send(swap(dy))

        def pass_on(dy):
            value = make(yof(dy) * 2 + k)
            swap(dy).wait_recv()
            ysend[dy - 1] = (value + drecv[dy].astype(f32)).astype(bf)
            send(rcopy(ysend.at[dy - 1], yrecv.at[dy - 1], y_ss.at[dy - 1], y_rs.at[dy - 1], vocab=yof(dy) * 2 + k))

        def keep():
            value = make(v)
            swap(0).wait_recv()
            out[...] = value + drecv[0].astype(f32)

        def finish():
            value = out[...]
            for dy in range(1, Y):
                rcopy(ysend.at[dy - 1], yrecv.at[dy - 1], y_ss.at[dy - 1], y_rs.at[dy - 1], vocab=v).wait_recv()
                value = value + yrecv[dy - 1].astype(f32)
            return value

        return give, pass_on, keep, finish

    give, pass_on, keep, finish = reduce_over(
        feature_part, facc, fsend, frecv, fysend, fyrecv, fd_ss, fd_rs, fy_ss, fy_rs
    )
    for dy in range(1, Y):
        give(dy)
        ring(1)
        pass_on(dy)
        ring(1)
    give(0)
    ring(1)
    keep()
    ring(4)
    tanh_value = tl[...].reshape(S, cols)
    pre = (finish() * (1.0 - tanh_value * tanh_value)).astype(bf)
    pre_ref[...] = pre.reshape(Z, G, cols)

    give, pass_on, keep, finish = reduce_over(
        slot_part, facc, sfsend, sfrecv, sfysend, sfyrecv, sd_ss, sd_rs, sy_ss, sy_rs
    )
    for dy in range(1, Y):
        give(dy)
        pass_on(dy)
        ring(1)
    give(0)
    keep()
    ring(5)
    ss[...] = finish().reshape(Z, G, cols)

    for i in range(Z):
        zz = zof(i)
        tokens = lax.dot_general(
            dmat[zz].astype(f32), ss[zz], (((0,), (0,)), ((), ())), precision=HIGHEST, preferred_element_type=f32
        )
        if i == 0:
            town[...] = tokens
        asend[i] = tokens.astype(bf)
        for r in range(2):
            if (i, r) != (0, 0):
                rows = pl.ds(pl.multiple_of(lax.rem(x + r, 2) * T, T), T)
                send(rcopy(asend.at[i, rows, :], ain.at[i, r], t_ss.at[i, r], t_rs.at[i, r], comp=comp_to(i, r)))
    ring((C - 2) * NS)
    home = town[xrow, :] + pback[xrow, :]
    for i, r in comp_peers:
        rcopy(asend.at[i, xrow, :], ain.at[i, r], t_ss.at[i, r], t_rs.at[i, r], comp=c).wait_recv()
        home = home + ain[i, r].astype(f32)
    gh_ref[...] = home

    def last(j, carry):
        at = pl.ds(pl.multiple_of(j * WORDS, WORDS), WORDS)
        for way in range(2):
            value = partial(way, C - 1, j)
            ring_copy(way, C - 2, j).wait_recv()
            ge_ref[way * R : (way + 1) * R, at] = (rbuf[way, C - 1, j].astype(f32) + value).astype(bf)
        return carry

    lax.fori_loop(0, NS, last, 0)

    for copy in sends:
        copy.wait_send()

    def drain(q, carry):
        s, j = lax.div(q, NS), lax.rem(q, NS)
        for way in range(2):
            ring_copy(way, s, j).wait_send()
        return carry

    lax.fori_loop(0, (C - 1) * NS, drain, 0)


def fused(owners, slices, hidden, routes, targets, saved_lse, target_logprob, prior_weight, projection, embedding):
    tok_dev, width = hidden.shape
    top = routes.shape[1]
    comp_dev, _, cols = projection.shape
    words = embedding.shape[1]
    experts = comp_dev * owners
    cap = capacity_of(owners, hidden, routes, projection)
    C, V, L, T, K, D = owners, slices, comp_dev, tok_dev, experts, width
    Z, Y, NS = C // 2, V // 2, words // WORDS
    G, R = L * 2 * cap, D // C // 2
    bf, f32 = jnp.bfloat16, jnp.float32
    small = jnp.concatenate(
        [routes.T.astype(f32), saved_lse.T, target_logprob.T, targets[None, :].astype(f32)], axis=0
    )
    small = jnp.concatenate([small, small], axis=1)
    dma = pltpu.SemaphoreType.DMA
    vm = pltpu.VMEM
    rows_b = 3 * K + 8
    scratch = [
        vm((L, D, cols), bf), vm((D, words), bf), vm((Z, 2 * T, D), bf),
        vm((K, 2 * T), f32), vm((C, K, 2 * T), f32), vm((rows_b, 2 * T), f32), vm((C, rows_b, 2 * T), f32),
        vm((V, K, cols), bf), vm((Z, G, 2 * T), bf), vm((3, Z, G, 1), f32), vm((Z, G, cols), f32),
        vm((V, Z, G, cols), bf), vm((D, Z * G), bf), vm((NS, Z * G, WORDS), f32), vm((NS, Z * G, WORDS), bf),
        vm((2, C, NS, R, WORDS), bf), vm((2, R, WORDS), f32), vm((Z * G, cols), f32),
        vm((Y, Z * G, cols), bf), vm((Y, Z * G, cols), bf),
        vm((max(1, Y - 1), Z * G, cols), bf), vm((max(1, Y - 1), Z * G, cols), bf),
        vm((Y, Z * G, cols), bf), vm((Y, Z * G, cols), bf),
        vm((max(1, Y - 1), Z * G, cols), bf), vm((max(1, Y - 1), Z * G, cols), bf),
        vm((Z, G, cols), f32), vm((Z, 2 * T, cols), bf), vm((Z, 2, T, cols), bf), vm((2 * T, cols), f32),
        vm((2 * T, cols), f32),
        dma((2,)), dma((C,)), dma((C,)), dma((C,)), dma((C,)), dma((V,)), dma((V,)), dma((Z,)), dma((Z,)),
        dma((Z,)), dma((Z,)), dma((Z, 2)), dma((Z, 2)),
        dma((Z,)), dma((Z,)), dma((Y, Z)), dma((Y, Z)), dma((Y, Z)), dma((Y, Z)), dma((2, C, NS)), dma((2, C, NS)),
        dma((Y,)), dma((Y,)), dma((Y,)), dma((Y,)), dma((Y,)), dma((Y,)), dma((Y,)), dma((Y,)),
        dma((Z, 2)), dma((Z, 2)),
    ]
    in_vmem = pl.BlockSpec(memory_space=pltpu.VMEM)
    anywhere = pl.BlockSpec(memory_space=pl.ANY)
    grad_hidden, prior_t, grad_embedding, slot_inputs, pre_grads = pl.pallas_call(
        functools.partial(kernel, (C, V, L, cap, top, K)),
        out_shape=(
            jax.ShapeDtypeStruct((T, cols), f32),
            jax.ShapeDtypeStruct((K, cols), f32),
            jax.ShapeDtypeStruct((D // C, words), bf),
            jax.ShapeDtypeStruct((Z, G, D), bf),
            jax.ShapeDtypeStruct((Z, G, cols), bf),
        ),
        in_specs=[in_vmem, in_vmem, in_vmem, anywhere, anywhere],
        out_specs=(in_vmem,) * 5,
        scratch_shapes=scratch,
        compiler_params=pltpu.CompilerParams(
            collective_id=0, has_side_effects=True, vmem_limit_bytes=67043328
        ),
    )(hidden, small, prior_weight.T, projection, embedding)
    per_comp = lambda a: jnp.swapaxes(a.reshape(Z, L, 2 * cap, a.shape[-1]), 0, 1).reshape(L, Z * 2 * cap, a.shape[-1])
    grad_projection = jnp.einsum(
        "lrd,lre->lde", per_comp(slot_inputs), per_comp(pre_grads), preferred_element_type=f32
    ).astype(bf)
    return grad_hidden, prior_t.T, grad_projection, grad_embedding


def solution(mesh):
    owners, slices = mesh.shape["comp"], mesh.shape["vocab"]

    def body(hidden, routes, targets, saved_lse, target_logprob, prior_weight, projection, embedding):
        args = (hidden, routes, targets, saved_lse, target_logprob, prior_weight, projection, embedding)
        if fits(owners, slices, hidden, routes, projection, embedding):
            return fused(owners, slices, *args)
        return shards(*args)

    return jax.shard_map(
        body,
        mesh=mesh,
        in_specs=(
            P("comp", None),
            P("comp", None),
            P("comp"),
            P("comp", None),
            P("comp", None),
            P("vocab", None),
            P("comp", None, "vocab"),
            P(None, "vocab"),
        ),
        out_specs=(
            P("comp", "vocab"),
            P("vocab", None),
            P("comp", None, "vocab"),
            P("comp", "vocab"),
        ),
        check_vma=False,
    )
```

```python
import functools

import jax
import jax.numpy as jnp
from jax import lax
from jax.experimental import pallas as pl
from jax.experimental.pallas import tpu as pltpu
from jax.sharding import PartitionSpec as P

MESH = pl.DeviceIdType.MESH
HIGHEST = lax.Precision.HIGHEST
WORDS = 512


def core_swap(value, count):
    return lax.ppermute(value, "vocab", [(i, i ^ 1) for i in range(count)])


def vocab_gather(block, count):
    me = lax.axis_index("vocab")
    pairs = count // 2
    ring = [(i, (i + 2) % count) for i in range(count)]
    held = [block]
    for _ in range(pairs - 1):
        held.append(lax.ppermute(held[-1], "vocab", ring))
    own = jnp.stack(held)
    other = core_swap(own, count)
    core = me % 2
    both = jnp.where(core == 0, jnp.stack([own, other], 1), jnp.stack([other, own], 1))
    if pairs == 2:
        order = jnp.where(me // 2 == 0, both, both[::-1])
    else:
        order = jnp.take(both, (me // 2 - jnp.arange(pairs)) % pairs, axis=0)
    return order.reshape((count,) + block.shape)


def vocab_scatter(blocks, count, wire):
    me = lax.axis_index("vocab")
    pairs = count // 2
    core, row = me % 2, me // 2
    split = blocks.reshape((pairs, 2) + blocks.shape[1:])
    mine = jnp.where(core == 0, split[:, 0], split[:, 1])
    theirs = jnp.where(core == 0, split[:, 1], split[:, 0])
    mine = mine + core_swap(theirs.astype(wire), count).astype(jnp.float32)
    ring = [(i, (i + 2) % count) for i in range(count)]
    total = lax.dynamic_index_in_dim(mine, (row - 1) % pairs, 0, keepdims=False)
    for step in range(1, pairs):
        got = lax.ppermute(total.astype(wire), "vocab", ring).astype(jnp.float32)
        total = got + lax.dynamic_index_in_dim(mine, (row - 1 - step) % pairs, 0, keepdims=False)
    return total


def comp_scatter(z_rows, grad_rows, owners, wire):
    me = lax.axis_index("comp")
    order = list(range(0, owners, 2)) + list(range(1, owners, 2))[::-1]
    place_of = [order.index(i) for i in range(owners)]
    place = jnp.array(place_of, jnp.int32)[me]
    order_array = jnp.array(order, jnp.int32)
    rows = z_rows.shape[1] // owners
    half = rows // 2

    def part(sign, step):
        owner = order_array[(place - sign * (1 + step)) % owners]
        start = owner * rows + (0 if sign == 1 else half)
        block = lax.dynamic_slice_in_dim(z_rows, start, half, 1)
        return lax.dot_general(
            block, grad_rows, (((0,), (0,)), ((), ())), preferred_element_type=jnp.float32
        )

    totals = []
    rings = [
        (sign, [(order[p], order[(p + sign) % owners]) for p in range(owners)]) for sign in (1, -1)
    ]
    totals = [part(sign, 0) for sign, _ in rings]
    for step in range(1, owners):
        moved = [
            lax.ppermute(total.astype(wire), "comp", ring) for total, (_, ring) in zip(totals, rings)
        ]
        totals = [
            got.astype(jnp.float32) + part(sign, step) for got, (sign, _) in zip(moved, rings)
        ]
    return jnp.concatenate(totals, axis=0)


def shards(hidden, routes, targets, saved_lse, target_logprob, prior_weight, projection, embedding):
    highest = lax.Precision.HIGHEST
    tok_dev, model_width = hidden.shape
    top = routes.shape[1]
    comp_dev = projection.shape[0]
    cols = projection.shape[2]
    voc_dev = embedding.shape[1]
    owners = lax.axis_size("comp")
    slices = lax.axis_size("vocab")
    experts_all = comp_dev * owners
    capacity = max(2, (2 * tok_dev * top + experts_all - 1) // experts_all)
    slot_rows = owners * capacity
    comp_index = lax.axis_index("comp")
    vocab_index = lax.axis_index("vocab")
    wire = jnp.bfloat16 if owners <= 8 else jnp.float32

    own_cols = lax.dynamic_slice_in_dim(hidden, vocab_index * cols, cols, 1)
    cols_all = lax.all_gather(own_cols, "comp", axis=0, tiled=True)
    hidden_all = vocab_gather(cols_all, slices)

    partial_logits = jnp.dot(own_cols, prior_weight, preferred_element_type=jnp.float32)
    prior_logits = lax.psum(partial_logits, "vocab")
    comp_ids = jnp.arange(experts_all, dtype=jnp.int32)
    picked = (routes[:, :, None] == comp_ids[None, None, :]).astype(jnp.float32)
    selected = jnp.sum(picked * prior_logits[:, None, :], axis=2)
    gate = jax.nn.softmax(selected, axis=-1)
    posterior = jax.nn.softmax(jax.nn.log_softmax(selected, axis=-1) + target_logprob, axis=-1)
    prior_grads = jnp.sum((gate - posterior)[:, :, None] * picked, axis=1)
    prior_back = lax.dot_general(
        prior_grads, prior_weight.astype(jnp.float32), (((1,), (1,)), ((), ())), precision=highest
    )
    packed = jnp.concatenate(
        [
            posterior,
            saved_lse,
            jnp.repeat(targets.astype(jnp.float32)[:, None], top, axis=1),
            routes.astype(jnp.float32),
            prior_grads,
        ],
        axis=1,
    )
    packed_all = lax.all_gather(packed, "comp", axis=0, tiled=True)
    grad_prior = lax.dot_general(
        cols_all.astype(jnp.float32),
        packed_all[:, 4 * top :],
        (((0,), (0,)), ((), ())),
        precision=highest,
    )

    pairs = tok_dev * top

    def pair_values(index):
        return packed_all[:, index * top : (index + 1) * top].reshape(owners, pairs)

    pair_comp = pair_values(3)
    own_ids = (comp_index * comp_dev + jnp.arange(comp_dev, dtype=jnp.int32)).astype(jnp.float32)
    hit = pair_comp[None, :, :] == own_ids[:, None, None]
    pair_ids = jnp.arange(pairs, dtype=jnp.int32)
    before = (pair_ids[:, None] < pair_ids[None, :]).astype(jnp.bfloat16)
    rank = jnp.einsum(
        "lbp,pq->lbq", hit.astype(jnp.bfloat16), before, preferred_element_type=jnp.float32
    )
    place = jnp.where(hit, rank, -1.0)
    slot_ids = jnp.arange(capacity, dtype=jnp.int32).astype(jnp.float32)
    dispatch = (place[:, :, None, :] == slot_ids[None, None, :, None]).astype(jnp.float32)

    def to_slots(index):
        values = pair_values(index)
        return jnp.sum(dispatch * values[None, :, None, :], axis=3).reshape(comp_dev * slot_rows)

    post_rows, lse_rows = to_slots(0), to_slots(1)
    target_rows = to_slots(2).astype(jnp.int32)
    fold = (pair_ids[:, None] // top == jnp.arange(tok_dev, dtype=jnp.int32)[None, :]).astype(jnp.bfloat16)
    token_hit = jnp.einsum(
        "lbsp,pt->lbst", dispatch.astype(jnp.bfloat16), fold, preferred_element_type=jnp.float32
    ).astype(jnp.bfloat16)

    rows_in = jnp.einsum(
        "lbst,kbtd->lbskd",
        token_hit,
        hidden_all.reshape(slices, owners, tok_dev, cols),
        preferred_element_type=jnp.float32,
    ).astype(jnp.bfloat16).reshape(comp_dev, slot_rows, model_width)
    preact = jnp.einsum("lrd,lde->lre", rows_in, projection, preferred_element_type=jnp.float32)
    tanh_value = jnp.tanh(preact)
    z_local = tanh_value.astype(jnp.bfloat16).reshape(comp_dev * slot_rows, cols)
    z_blocks = vocab_gather(z_local, slices)
    z_all = jnp.swapaxes(z_blocks, 0, 1).reshape(comp_dev * slot_rows, slices * cols)
    logits = jnp.dot(z_all, embedding, preferred_element_type=jnp.float32)
    vocab_ids = vocab_index * voc_dev + jnp.arange(voc_dev, dtype=jnp.int32)
    target_hit = (target_rows[:, None] == vocab_ids[None, :]).astype(jnp.float32)
    logit_grads = (post_rows[:, None] * (jnp.exp(logits - lse_rows[:, None]) - target_hit)).astype(
        jnp.bfloat16
    )
    logit_grads = lax.optimization_barrier(logit_grads)
    feature_parts = jnp.einsum(
        "rv,kdv->krd",
        logit_grads,
        embedding.reshape(slices, cols, voc_dev),
        preferred_element_type=jnp.float32,
    )
    feature_grads = vocab_scatter(feature_parts, slices, wire).reshape(comp_dev, slot_rows, cols)
    pre_grads = (feature_grads * (1.0 - tanh_value * tanh_value)).astype(jnp.bfloat16)
    slot_parts = jnp.einsum(
        "lre,lkde->klrd",
        pre_grads,
        projection.reshape(comp_dev, slices, model_width // slices, cols),
        preferred_element_type=jnp.float32,
    )
    slot_share = vocab_scatter(slot_parts, slices, wire)
    token_parts = jnp.einsum(
        "lbst,lbsd->btd",
        token_hit.astype(jnp.float32),
        slot_share.reshape(comp_dev, owners, capacity, model_width // slices),
        precision=highest,
    )
    returned = lax.all_to_all(
        token_parts.astype(wire), "comp", split_axis=0, concat_axis=0, tiled=True
    )
    grad_hidden = jnp.sum(returned.astype(jnp.float32), axis=0) + prior_back
    grad_projection = jnp.einsum(
        "lrd,lre->lde", rows_in, pre_grads, preferred_element_type=jnp.float32
    ).astype(jnp.bfloat16)
    grad_embedding = comp_scatter(z_all, logit_grads, owners, wire).astype(jnp.bfloat16)
    return (grad_hidden, grad_prior, grad_projection, grad_embedding)


def capacity_of(owners, hidden, routes, projection):
    tok_dev, top = hidden.shape[0], routes.shape[1]
    experts_all = projection.shape[0] * owners
    return max(2, (2 * tok_dev * top + experts_all - 1) // experts_all)


def fits(owners, slices, hidden, routes, projection, embedding):
    capacity = capacity_of(owners, hidden, routes, projection)
    rows = hidden.shape[1] // owners
    return (
        owners % 4 == 0
        and slices % 2 == 0
        and capacity % 16 == 0
        and (2 * hidden.shape[0]) % 128 == 0
        and rows % 32 == 0
        and embedding.shape[1] % (2 * WORDS) == 0
        and projection.shape[2] % 128 == 0
    )


def nt_dot(a, b):
    return lax.dot_general(a, b, (((1,), (1,)), ((), ())), preferred_element_type=jnp.float32)


def kernel(
    dims,
    hidden_ref, routes_ref, lse_ref, tlp_ref, target_ref, pw_ref, proj_hbm, emb_hbm,
    gh_ref, gprior_ref, ge_ref, xt_ref, pre_ref,
    xs_ref, proj, emb, hid, infoa_out, infoa, infob_out, infob, pwall, dmat, cols3, tl, zall, zt, lacc, lg,
    xsend, xrecv, z1recv, z2recv, facc, fds, fdr, yas, yar, zas, zar, zbs, zbr, ybs, ybr,
    sds, sdr, sys, syr, ss, sacc, tokp, txs, txr, tzs, tzr, pback,
    load_sem, a_ss, a_rs, b_ss, b_rs, pw_ss, pw_rs, hz_ss, hz_rs, hx_ss, hx_rs, hd_ss, hd_rs,
    zd_ss, zd_rs, zy_ss, zy_rs, zf_ss, zf_rs, zz_ss, zz_rs, x_ss, x_rs, z1_ss, z1_rs, z2_ss, z2_rs,
    fd_ss, fd_rs, ya_ss, ya_rs, za_ss, za_rs, zb_ss, zb_rs, yb_ss, yb_rs,
    sd_ss, sd_rs, sy_ss, sy_rs, tx_ss, tx_rs, tz_ss, tz_rs,
):
    C, V, L, cap, top, K = dims
    Z, Y = C // 2, V // 2
    T, D = hidden_ref.shape
    cols = pw_ref.shape[1]
    W = emb_hbm.shape[1]
    WH = W // 2
    NJ = WH // WORDS
    NU = 2 * NJ
    G = L * 2 * cap
    S = Z * G
    half = D // 2
    R2 = D // C
    R = R2 // 2
    T2 = 2 * T
    bf, f32 = jnp.bfloat16, jnp.float32

    c, v = lax.axis_index("comp"), lax.axis_index("vocab")
    z, x = lax.div(c, 2), lax.rem(c, 2)
    y, k = lax.div(v, 2), lax.rem(v, 2)
    xo, ko = 1 - x, 1 - k
    partner = y * 2 + ko
    sw = lax.rem(z, 2)
    zp = z + 1 - 2 * sw
    pair = zp * 2 + x

    def zof(i):
        return lax.rem(z + i, Z)

    def zback(i):
        return lax.rem(z + Z - i, Z)

    def near_z(at, i):
        if Z != 4:
            return lax.rem(at + Z - i, Z)
        if i % 2:
            at = at + 1 - 2 * lax.rem(at, 2)
        if i // 2:
            at = at + 2 - 4 * lax.div(at, 2)
        return at

    def zto(i):
        return near_z(z, i) if Z == 4 else zof(i)

    def zfrom(i):
        return near_z(z, i)

    def yof(i):
        return lax.rem(y + i, Y)

    def yback(i):
        return lax.rem(y + Y - i, Y)

    def rcopy(src, dst, ss_, rs_, **dev):
        return pltpu.make_async_remote_copy(
            src_ref=src, dst_ref=dst, send_sem=ss_, recv_sem=rs_, device_id=dev, device_id_type=MESH
        )

    sends = []

    def send(copy):
        copy.start()
        sends.append(copy)

    load_p = pltpu.make_async_copy(proj_hbm, proj, load_sem.at[0])
    load_e = pltpu.make_async_copy(emb_hbm.at[:, pl.ds(pl.multiple_of(sw * WH, WH), WH)], emb, load_sem.at[1])
    load_p.start()
    load_e.start()

    comp_peers = [(i, r) for i in range(Z) for r in range(2) if (i, r) != (0, 0)]
    vocab_peers = [(i, r) for i in range(Y) for r in range(2) if (i, r) != (0, 0)]

    def comp_to(i, r):
        return zof(i) * 2 + lax.rem(x + r, 2)

    def comp_from(i, r):
        return zback(i) * 2 + lax.rem(x + r, 2)

    def vocab_to(i, r):
        return yof(i) * 2 + lax.rem(k + r, 2)

    def vocab_from(i, r):
        return yback(i) * 2 + lax.rem(k + r, 2)

    barrier = pltpu.get_barrier_semaphore()
    for dy in range(1, Y):
        pl.semaphore_signal(
            barrier, inc=1, device_id={"comp": pair, "vocab": yof(dy) * 2 + k}, device_id_type=MESH
        )
    for i, r in comp_peers:
        pl.semaphore_signal(barrier, inc=1, device_id={"comp": comp_to(i, r)}, device_id_type=MESH)
    for i, r in vocab_peers:
        pl.semaphore_signal(barrier, inc=1, device_id={"vocab": vocab_to(i, r)}, device_id_type=MESH)

    lane = lax.broadcasted_iota(jnp.int32, (K, T2), 1)
    mine = (lane >= x * T) & (lane < x * T + T)
    comp_id = lax.broadcasted_iota(jnp.int32, (K, T2), 0).astype(f32)
    hit = jnp.zeros((K, T2), f32)
    lse_k = jnp.zeros((K, T2), f32)
    tlp_k = jnp.zeros((K, T2), f32)

    def both(ref):
        value = ref[...].astype(f32)
        return jnp.concatenate([value, value], axis=1)

    route, lse_in, tlp_in, target_in = both(routes_ref), both(lse_ref), both(tlp_ref), both(target_ref)
    for j in range(top):
        named = (route[j : j + 1, :] == comp_id) & mine
        hit = jnp.where(named, 1.0, hit)
        lse_k = jnp.where(named, lse_in[j : j + 1, :], lse_k)
        tlp_k = jnp.where(named, tlp_in[j : j + 1, :], tlp_k)
    on = hit > 0.5
    upper = (
        lax.broadcasted_iota(jnp.int32, (T2, T2), 0) < lax.broadcasted_iota(jnp.int32, (T2, T2), 1)
    ).astype(f32).astype(bf)
    rank = jnp.dot(hit.astype(bf), upper, preferred_element_type=f32)
    place = jnp.where(on, rank, -1.0)
    infoa_out[...] = place
    hid[z, pl.ds(pl.multiple_of(x * T, T), T), :] = hidden_ref[...]
    pwall[v] = pw_ref[...]
    pl.semaphore_wait(barrier, len(comp_peers) + len(vocab_peers) + Y - 1)

    xrow = pl.ds(pl.multiple_of(x * T, T), T)
    xorow = pl.ds(pl.multiple_of(xo * T, T), T)
    kcol = pl.ds(pl.multiple_of(k * half, half), half)
    kocol = pl.ds(pl.multiple_of(ko * half, half), half)
    for i, r in comp_peers:
        n = i * 2 + r
        send(rcopy(infoa_out, infoa.at[c], a_ss.at[n], a_rs.at[n], comp=comp_to(i, r)))
    send(rcopy(hidden_ref.at[:, kcol], hid.at[z, xrow, kcol], hx_ss.at[0], hx_rs.at[0], comp=z * 2 + xo))
    for i in range(1, Z):
        send(rcopy(hidden_ref.at[:, kcol], hid.at[z, xrow, kcol], hz_ss.at[i], hz_rs.at[i], comp=zto(i) * 2 + x))
    for i, r in vocab_peers:
        n = i * 2 + r
        send(rcopy(pw_ref, pwall.at[v], pw_ss.at[n], pw_rs.at[n], vocab=vocab_to(i, r)))
    infoa[c] = place

    for i, r in vocab_peers:
        n = i * 2 + r
        rcopy(pw_ref, pwall.at[vocab_from(i, r)], pw_ss.at[n], pw_rs.at[n], vocab=vocab_from(i, r)).wait_recv()
    logit = jnp.zeros((K, T), f32)
    for vv in range(V):
        logit = logit + nt_dot(pwall[vv], hidden_ref[:, vv * cols : (vv + 1) * cols])
    logit = jnp.concatenate([logit, logit], axis=1)

    def top_of(values):
        return jnp.max(jnp.where(on, values, -1e30), axis=0, keepdims=True)

    def norm(values):
        total = jnp.sum(values, axis=0, keepdims=True)
        return jnp.where(total > 0.0, total, 1.0)

    shifted = logit - top_of(logit)
    weight = jnp.where(on, jnp.exp(jnp.where(on, shifted, 0.0)), 0.0)
    total = norm(weight)
    gate = weight / total
    mixed = shifted - jnp.log(total) + tlp_k
    mixed = jnp.where(on, mixed - top_of(mixed), 0.0)
    weight = jnp.where(on, jnp.exp(mixed), 0.0)
    post = weight / norm(weight)
    pgrad = gate - post
    target = jnp.where(mine[0:8], jnp.broadcast_to(target_in, (8, T2)), 0.0)
    infob_value = jnp.concatenate([post, lse_k, pgrad, target], axis=0)
    infob_out[...] = infob_value
    infob[c] = infob_value
    for i, r in comp_peers:
        n = i * 2 + r
        send(rcopy(infob_out, infob.at[c], b_ss.at[n], b_rs.at[n], comp=comp_to(i, r)))
    pback[...] = lax.dot_general(
        pgrad, pw_ref[...].astype(f32), (((0,), (0,)), ((), ())), precision=HIGHEST, preferred_element_type=f32
    )

    for i, r in comp_peers:
        n = i * 2 + r
        rcopy(infoa_out, infoa.at[comp_from(i, r)], a_ss.at[n], a_rs.at[n], comp=comp_from(i, r)).wait_recv()
    slot_id = lax.broadcasted_iota(jnp.int32, (cap, T2), 0).astype(f32)
    for zz in range(Z):
        for l in range(L):
            for xx in range(2):
                row = infoa[zz * 2 + xx, pl.ds(c * L + l, 1), :]
                start = l * 2 * cap + xx * cap
                dmat[zz, start : start + cap, :] = (row == slot_id).astype(f32).astype(bf)

    def forward(i):
        if i > 0:
            rcopy(hidden_ref.at[:, kcol], hid.at[zfrom(i), xrow, kcol], hz_ss.at[i], hz_rs.at[i], comp=c).wait_recv()
            piece = hid.at[zfrom(i), xrow, kcol]
            send(rcopy(piece, piece, hx_ss.at[i], hx_rs.at[i], comp=z * 2 + xo))
            send(rcopy(piece, piece, hd_ss.at[i, 0], hd_rs.at[i, 0], vocab=partner))

    def forward_x(i):
        piece = hid.at[zfrom(i), xorow, kcol]
        rcopy(piece, piece, hx_ss.at[i], hx_rs.at[i], comp=z * 2 + xo).wait_recv()
        send(rcopy(piece, piece, hd_ss.at[i, 1], hd_rs.at[i, 1], vocab=partner))

    def arrive(i):
        if i > 0:
            piece = hid.at[zfrom(i), xrow, kocol]
            rcopy(piece, piece, hd_ss.at[i, 0], hd_rs.at[i, 0], vocab=partner).wait_recv()
        piece = hid.at[zfrom(i), xorow, kocol]
        rcopy(piece, piece, hd_ss.at[i, 1], hd_rs.at[i, 1], vocab=partner).wait_recv()

    def zpair(i):
        return near_z(zp, i)

    def spread(side, i):
        piece = zall.at[side, v, zfrom(i) if side == 0 else zpair(i)]
        for dy in range(1, Y):
            if (side, i) != (1, Z - 1):
                send(rcopy(piece, piece, zy_ss.at[side, dy, i], zy_rs.at[side, dy, i], vocab=yof(dy) * 2 + k))
        send(rcopy(piece, piece, zd_ss.at[side, i], zd_rs.at[side, i], vocab=partner))

    def project(i):
        zz = zfrom(i)
        rows = jnp.dot(dmat[zz], hid[zz], preferred_element_type=f32).astype(bf)
        xs_ref[zz] = rows
        for l in range(L):
            span = slice(l * 2 * cap, (l + 1) * 2 * cap)
            value = jnp.tanh(jnp.dot(rows[span], proj[l], preferred_element_type=f32))
            tl[zz, span, :] = value
            zall[0, v, zz, span, :] = value.astype(bf)
        if i == Z - 1:
            for dy in range(1, Y):
                send(rcopy(
                    zall.at[0, v, zz], zall.at[1, v, zz], zy_ss.at[1, dy, i], zy_rs.at[1, dy, i],
                    comp=pair, vocab=yof(dy) * 2 + k,
                ))
        send(rcopy(zall.at[0, v, zz], zall.at[1, v, zz], zz_ss.at[i], zz_rs.at[i], comp=pair))
        spread(0, i)

    def relay(i):
        rcopy(zall.at[0, v, zpair(i)], zall.at[1, v, zpair(i)], zz_ss.at[i], zz_rs.at[i], comp=pair).wait_recv()
        spread(1, i)

    def cross(side, i):
        for dy in range(1, Y):
            piece = zall.at[side, yback(dy) * 2 + k, zfrom(i) if side == 0 else zpair(i)]
            rcopy(piece, piece, zy_ss.at[side, dy, i], zy_rs.at[side, dy, i], vocab=v).wait_recv()
            send(rcopy(piece, piece, zf_ss.at[side, dy, i], zf_rs.at[side, dy, i], vocab=partner))

    def zdone(side, i):
        piece = zall.at[side, partner, zfrom(i) if side == 0 else zpair(i)]
        rcopy(piece, piece, zd_ss.at[side, i], zd_rs.at[side, i], vocab=partner).wait_recv()

    def crossed(side, i):
        for dy in range(1, Y):
            piece = zall.at[side, yback(dy) * 2 + ko, zfrom(i) if side == 0 else zpair(i)]
            rcopy(piece, piece, zf_ss.at[side, dy, i], zf_rs.at[side, dy, i], vocab=partner).wait_recv()

    forward_x(0)
    if Z > 1:
        forward(1)
    load_p.wait()
    arrive(0)
    project(0)
    for i in range(1, Z):
        forward_x(i)
        if i + 1 < Z:
            forward(i + 1)
        arrive(i)
        project(i)
        relay(i - 1)

    for i, r in comp_peers:
        n = i * 2 + r
        rcopy(infob_out, infob.at[comp_from(i, r)], b_ss.at[n], b_rs.at[n], comp=comp_from(i, r)).wait_recv()
    for side in range(2):
        base = (c if side == 0 else pair) * L
        for zz in range(Z):
            for l in range(L):
                for xx in range(2):
                    b = zz * 2 + xx
                    start = l * 2 * cap + xx * cap
                    pick = infoa[b, pl.ds(base + l, 1), :] == slot_id
                    rows3 = (
                        infob[b, pl.ds(base + l, 1), :],
                        infob[b, pl.ds(K + base + l, 1), :],
                        infob[b, 3 * K : 3 * K + 1, :],
                    )
                    for q in range(3):
                        cols3[q, side, zz, start : start + cap, :] = jnp.sum(
                            jnp.where(pick, rows3[q], 0.0), axis=1, keepdims=True
                        )
    relay(Z - 1)
    owncols = pl.ds(pl.multiple_of(v * cols, cols), cols)
    gp = jnp.zeros((K, cols), f32)
    for zz in range(Z):
        grads = infob[zz * 2, 2 * K : 3 * K, :] + infob[zz * 2 + 1, 2 * K : 3 * K, :]
        gp = gp + jnp.dot(grads, hid[zz, :, owncols].astype(f32), precision=HIGHEST, preferred_element_type=f32)
    gprior_ref[...] = gp
    load_e.wait()

    def features(vv):
        return zall[:, vv].reshape(2 * S, cols)

    def feature_rows(vv):
        return pl.ds(pl.multiple_of(vv * cols, cols), cols)

    def turn_features(vv):
        for side in range(2):
            zt[feature_rows(vv), side * S : (side + 1) * S] = zall[side, vv].reshape(S, cols).T

    for i in range(Z):
        zdone(0, i)
    for i in range(Z - 1):
        cross(0, i)
    for i in range(Z - 1):
        zdone(1, i)
    cross(0, Z - 1)
    cross(1, 0)
    zdone(1, Z - 1)

    def early(j, carry):
        at = pl.ds(pl.multiple_of(j * WORDS, WORDS), WORDS)
        lacc[j] = jnp.dot(
            features(v), emb[feature_rows(v), at], preferred_element_type=f32
        ) + jnp.dot(features(partner), emb[feature_rows(partner), at], preferred_element_type=f32)
        return carry

    lax.fori_loop(0, NJ, early, 0)
    for kk in range(2):
        turn_features(y * 2 + kk)
    for i in range(1, Z):
        cross(1, i)
    for side in range(2):
        for i in range(Z):
            crossed(side, i)
    for dy in range(1, Y):
        for kk in range(2):
            turn_features(yof(dy) * 2 + kk)

    def owner_z(t):
        near = lax.rem(z + 2 * lax.rem(1 + lax.div(t, 2), Z // 2), Z)
        other = near + 1 - 2 * lax.rem(near, 2)
        e = 1 - lax.rem(t, 2)
        return e * other + (1 - e) * near

    def partial(xx, t, q):
        j, fh = lax.div(q, 2), lax.rem(q, 2)
        owner = owner_z(t) * 2 + xx
        rows = pl.ds(pl.multiple_of(owner * R2 + fh * R, R), R)
        return jnp.dot(zt[rows, :], lg[j], preferred_element_type=f32)

    def x_copy(t, q):
        return rcopy(xsend.at[t, q], xrecv.at[t, q], x_ss.at[t, q], x_rs.at[t, q], comp=z * 2 + xo)

    def z1_copy(t, q):
        goal = lax.rem(z + 2 * (1 + lax.div(t, 2)), Z) * 2 + x
        return rcopy(xrecv.at[t, q], z1recv.at[t, q], z1_ss.at[t, q], z1_rs.at[t, q], comp=goal)

    def z2_copy(q):
        return rcopy(xrecv.at[Z - 2, q], z2recv.at[q], z2_ss.at[q], z2_rs.at[q], comp=pair)

    def xput(n, carry):
        t, q = lax.div(n, NU), lax.rem(n, NU)
        xsend[t, q] = partial(xo, t, q).astype(bf)
        x_copy(t, q).start()
        return carry

    def far_event(n, carry):
        t, q = lax.div(n, NU), lax.rem(n, NU)
        value = partial(x, t, q)
        x_copy(t, q).wait_recv()
        xrecv[t, q] = (value + xrecv[t, q].astype(f32)).astype(bf)
        z1_copy(t, q).start()
        return carry

    def near_value(te, q):
        t = Z - 2 + te
        value = partial(x, t, q)
        x_copy(t, q).wait_recv()
        value = value + xrecv[t, q].astype(f32)
        for dp in range(Z // 2 - 1):
            z1_copy(2 * dp + te, q).wait_recv()
            value = value + z1recv[2 * dp + te, q].astype(f32)
        return value.astype(bf)

    def near_event(q, carry):
        xrecv[Z - 2, q] = near_value(0, q)
        z2_copy(q).start()
        return carry

    def place_of(q, half):
        j, fh = lax.div(q, 2), lax.rem(q, 2)
        return (
            pl.ds(pl.multiple_of(fh * R, R), R),
            pl.ds(pl.multiple_of(half * WH + j * WORDS, WORDS), WORDS),
        )

    def own_event(q, carry):
        rows, at = place_of(q, sw)
        ge_ref[rows, at] = near_value(1, q)
        return carry

    def last_event(q, carry):
        z2_copy(q).wait_recv()
        rows, at = place_of(q, 1 - sw)
        ge_ref[rows, at] = z2recv[q]
        return carry

    events = {"x": [0, Z * NU, xput], "far": [0, (Z - 2) * NU, far_event], "near": [0, NU, near_event],
              "own": [0, NU, own_event], "last": [0, NU, last_event]}

    inner = lax.div(lax.rem(z + 1, Z), 2) == 1
    far_total = (Z - 2) * NU
    done = {True: 0, False: 0}

    def run_far(group, count):
        start, end = done[group], min(done[group] + count, far_total)
        done[group] = end
        if end > start:
            @pl.when(inner if group else jnp.logical_not(inner))
            def _():
                lax.fori_loop(start, end, far_event, 0)

    def run(kind, count):
        entry = events[kind]
        end = min(entry[0] + count, entry[1])
        if end > entry[0]:
            lax.fori_loop(entry[0], end, entry[2], 0)
        entry[0] = end

    lse_rows = cols3[1].reshape(2 * S, 1)
    post_rows = cols3[0].reshape(2 * S, 1)
    target_rows = cols3[2].reshape(2 * S, 1).astype(jnp.int32)

    def words(j, carry):
        at = pl.ds(pl.multiple_of(j * WORDS, WORDS), WORDS)
        logits = lacc[j]
        for dy in range(1, Y):
            for kk in range(2):
                vv = yof(dy) * 2 + kk
                logits = logits + jnp.dot(features(vv), emb[feature_rows(vv), at], preferred_element_type=f32)
        ids = v * W + sw * WH + j * WORDS + lax.broadcasted_iota(jnp.int32, (2 * S, WORDS), 1)
        onehot = (target_rows == ids).astype(f32)
        lg[j] = (post_rows * (jnp.exp(logits - lse_rows) - onehot)).astype(bf)
        lax.fori_loop(2 * j, 2 * j + 2, xput, 0)
        return carry

    lax.fori_loop(0, NJ, words, 0)
    events["x"][0] = NU

    def feature_part(side, vv):
        def add(j, total):
            at = pl.ds(pl.multiple_of(j * WORDS, WORDS), WORDS)
            return total + nt_dot(lg[j, side * S : (side + 1) * S, :], emb[feature_rows(vv), at])

        total = nt_dot(lg[0, side * S : (side + 1) * S, :], emb[feature_rows(vv), 0:WORDS])
        for j in range(1, NJ):
            total = add(j, total)
        return total

    def feature_swap(side, dy):
        return rcopy(fds.at[side, dy], fdr.at[side, dy], fd_ss.at[side, dy], fd_rs.at[side, dy], vocab=partner)

    def give(side, dy):
        fds[side, dy] = feature_part(side, yof(dy) * 2 + ko).astype(bf)
        send(feature_swap(side, dy))

    def take(side, dy):
        value = feature_part(side, yof(dy) * 2 + k)
        feature_swap(side, dy).wait_recv()
        facc[side, dy] = value + fdr[side, dy].astype(f32)

    H = S // 2

    def ya_copy(side, dy):
        return rcopy(
            yas.at[side, dy - 1], yar.at[side, dy - 1], ya_ss.at[side, dy - 1], ya_rs.at[side, dy - 1],
            vocab=yof(dy) * 2 + k,
        )

    def yb_copy(dy):
        return rcopy(ybs.at[dy - 1], ybr.at[dy - 1], yb_ss.at[dy - 1], yb_rs.at[dy - 1], vocab=yof(dy) * 2 + k)

    def zb_copy(dy):
        return rcopy(zbs.at[dy], zbr.at[dy], zb_ss.at[dy], zb_rs.at[dy], comp=pair)

    za_copy = rcopy(zas, zar, za_ss.at[0], za_rs.at[0], comp=pair)

    def ya_out(side, dy):
        yas[side, dy - 1] = facc[side, dy, 0:H, :].astype(bf)
        send(ya_copy(side, dy))

    def zb_out(dy):
        zbs[dy] = facc[1, dy, H:S, :].astype(bf)
        send(zb_copy(dy))

    for dy in range(1, Y):
        give(1, dy)
        run("x", 1)
        run_far(True, 1)
        give(0, dy)
        run("x", 1)
        take(1, dy)
        ya_out(1, dy)
        zb_out(dy)
        run("x", 1)
        run_far(True, 1)
        take(0, dy)
        ya_out(0, dy)
        run("x", 1)
    give(1, 0)
    run("x", 2)
    run_far(True, 1)
    give(0, 0)
    run("x", 2)
    take(1, 0)
    zb_out(0)
    run("x", 2)
    take(0, 0)
    run("x", Z * NU)
    value = facc[1, 0, 0:H, :]
    for dy in range(1, Y):
        ya_copy(1, dy).wait_recv()
        value = value + yar[1, dy - 1].astype(f32)
    zas[...] = value.astype(bf)
    send(za_copy)
    run_far(True, 1)
    run_far(False, 4)

    def turned(d, carry):
        at = pl.ds(pl.multiple_of(d * cols, cols), cols)
        for l in range(L):
            rows = xs_ref[:, l * 2 * cap : (l + 1) * 2 * cap, at].reshape(Z * 2 * cap, cols)
            xt_ref[l, at, :] = rows.T
        return carry

    lax.fori_loop(0, V, turned, 0)
    for dy in range(1, Y):
        zb_copy(dy).wait_recv()
        ybs[dy - 1] = (facc[0, dy, H:S, :] + zbr[dy].astype(f32)).astype(bf)
        send(yb_copy(dy))
    run_far(True, 2)
    run_far(False, 2)
    low, high = facc[0, 0, 0:H, :], facc[0, 0, H:S, :]
    zb_copy(0).wait_recv()
    facc[0, 0, H:S, :] = high + zbr[0].astype(f32)
    for dy in range(1, Y):
        ya_copy(0, dy).wait_recv()
        low = low + yar[0, dy - 1].astype(f32)
    facc[0, 0, 0:H, :] = low
    run_far(True, far_total)
    run_far(False, far_total)
    low, high = facc[0, 0, 0:H, :], facc[0, 0, H:S, :]
    for dy in range(1, Y):
        yb_copy(dy).wait_recv()
        high = high + ybr[dy - 1].astype(f32)
    za_copy.wait_recv()
    low = low + zar[...].astype(f32)
    for n, total in enumerate((low, high)):
        zspan = slice(n * Z // 2, (n + 1) * Z // 2)
        tanh_value = tl[zspan].reshape(H, cols)
        pre_ref[zspan] = (total * (1.0 - tanh_value * tanh_value)).astype(bf).reshape(Z // 2, G, cols)

    def slot_part(vv):
        for l in range(L):
            span = slice(l * 2 * cap, (l + 1) * 2 * cap)
            rows = pre_ref[:, span, :].reshape(Z * 2 * cap, cols)
            ss[:, span, :] = nt_dot(rows, proj[l, feature_rows(vv), :]).reshape(Z, 2 * cap, cols)

    def slot_swap(dy):
        return rcopy(sds.at[dy], sdr.at[dy], sd_ss.at[dy], sd_rs.at[dy], vocab=partner)

    def sy_copy(dy, i):
        zz = zof(i)
        return rcopy(
            sys.at[dy - 1, zz], syr.at[dy - 1, zz], sy_ss.at[dy - 1, i], sy_rs.at[dy - 1, i], vocab=yof(dy) * 2 + k
        )

    order = list(range(1, Z)) + [0]
    for dy in range(1, Y):
        slot_part(yof(dy) * 2 + ko)
        sds[dy] = ss[...].astype(bf)
        send(slot_swap(dy))
        slot_part(yof(dy) * 2 + k)
        slot_swap(dy).wait_recv()
        for i in order:
            sys[dy - 1, zof(i)] = (ss[zof(i)] + sdr[dy, zof(i)].astype(f32)).astype(bf)
            send(sy_copy(dy, i))
    slot_part(partner)
    sds[0] = ss[...].astype(bf)
    send(slot_swap(0))
    slot_part(v)
    slot_swap(0).wait_recv()
    sacc[...] = ss[...] + sdr[0].astype(f32)
    run("near", 1)

    def tx_copy(i):
        return rcopy(txs.at[i], txr.at[i], tx_ss.at[i], tx_rs.at[i], comp=z * 2 + xo)

    def tz_copy(i):
        return rcopy(tzs.at[i], tzr.at[i], tz_ss.at[i], tz_rs.at[i], comp=zof(i) * 2 + x)

    def fold(i):
        zz = zof(i)
        value = sacc[zz]
        for dy in range(1, Y):
            sy_copy(dy, i).wait_recv()
            value = value + syr[dy - 1, zz].astype(f32)
        tokp[i] = lax.dot_general(
            dmat[zz].astype(f32), value, (((0,), (0,)), ((), ())), precision=HIGHEST, preferred_element_type=f32
        )
        txs[i] = tokp[i, xorow, :].astype(bf)
        send(tx_copy(i))

    def homeward(i):
        tx_copy(i).wait_recv()
        value = tokp[i, xrow, :] + txr[i].astype(f32)
        if i > 0:
            tzs[i] = value.astype(bf)
            send(tz_copy(i))
        return value

    for n, i in enumerate(order):
        fold(i)
        run("near", 1)
        if n > 0:
            homeward(order[n - 1])
    run("near", NU)
    home = homeward(order[-1]) + pback[xrow, :]
    run("own", NU - 1)
    for i in range(1, Z):
        tz_copy(i).wait_recv()
        home = home + tzr[i].astype(f32)
    gh_ref[...] = home
    run("own", NU)
    run("last", NU)

    for copy in sends:
        copy.wait_send()

    def drain_x(n, carry):
        x_copy(lax.div(n, NU), lax.rem(n, NU)).wait_send()
        return carry

    def drain_z1(n, carry):
        z1_copy(lax.div(n, NU), lax.rem(n, NU)).wait_send()
        return carry

    def drain_z2(q, carry):
        z2_copy(q).wait_send()
        return carry

    lax.fori_loop(0, Z * NU, drain_x, 0)
    lax.fori_loop(0, (Z - 2) * NU, drain_z1, 0)
    lax.fori_loop(0, NU, drain_z2, 0)


def finish_kernel(dims, gh_ref, gprior_ref, ge_ref, xt_ref, pre_ref, gh_out, gprior_out, ge_out, out, buf, sem, out_sem):
    L, Z, cap, chunk = dims
    copies = [
        pltpu.make_async_copy(ge_ref, ge_out, sem.at[0]),
        pltpu.make_async_copy(gh_ref, gh_out, sem.at[1]),
        pltpu.make_async_copy(gprior_ref, gprior_out, sem.at[2]),
    ]
    for copy in copies:
        copy.start()
    cols = pre_ref.shape[-1]
    for l in range(L):
        rows = pre_ref[:, l * 2 * cap : (l + 1) * 2 * cap, :].reshape(Z * 2 * cap, cols)
        for n in range(xt_ref.shape[1] // chunk):
            at = pl.ds(n * chunk, chunk)
            buf[l, at, :] = jnp.dot(xt_ref[l, at, :], rows, preferred_element_type=jnp.float32).astype(buf.dtype)
            copy = pltpu.make_async_copy(buf.at[l, at, :], out.at[l, at, :], out_sem.at[l, n])
            copy.start()
            copies.append(copy)
    for copy in copies:
        copy.wait()


def fused(owners, slices, hidden, routes, targets, saved_lse, target_logprob, prior_weight, projection, embedding):
    tok_dev, width = hidden.shape
    top = routes.shape[1]
    comp_dev, _, cols = projection.shape
    words = embedding.shape[1]
    experts = comp_dev * owners
    cap = capacity_of(owners, hidden, routes, projection)
    C, V, L, T, K, D = owners, slices, comp_dev, tok_dev, experts, width
    Z, Y = C // 2, V // 2
    G, R = L * 2 * cap, D // C // 2
    bf, f32 = jnp.bfloat16, jnp.float32
    dma = pltpu.SemaphoreType.DMA
    vm = pltpu.VMEM
    rows_b = 3 * K + 8
    S, H, NJ = Z * G, Z * G // 2, words // 2 // WORDS
    NU, Y1, far = 2 * NJ, max(1, Y - 1), max(1, Z - 2)
    scratch = [
        vm((Z, G, D), bf), vm((L, D, cols), bf), vm((D, words // 2), bf), vm((Z, 2 * T, D), bf),
        vm((K, 2 * T), f32), vm((C, K, 2 * T), f32), vm((rows_b, 2 * T), f32), vm((C, rows_b, 2 * T), f32),
        vm((V, K, cols), bf), vm((Z, G, 2 * T), bf), vm((3, 2, Z, G, 1), f32), vm((Z, G, cols), f32),
        vm((2, V, Z, G, cols), bf), vm((D, 2 * S), bf), vm((NJ, 2 * S, WORDS), f32), vm((NJ, 2 * S, WORDS), bf),
        vm((Z, NU, R, WORDS), bf), vm((Z, NU, R, WORDS), bf), vm((far, NU, R, WORDS), bf), vm((NU, R, WORDS), bf),
        vm((2, Y, S, cols), f32), vm((2, Y, S, cols), bf), vm((2, Y, S, cols), bf),
        vm((2, Y1, H, cols), bf), vm((2, Y1, H, cols), bf), vm((H, cols), bf), vm((H, cols), bf),
        vm((Y, H, cols), bf), vm((Y, H, cols), bf), vm((Y1, H, cols), bf), vm((Y1, H, cols), bf),
        vm((Y, Z, G, cols), bf), vm((Y, Z, G, cols), bf), vm((Y1, Z, G, cols), bf), vm((Y1, Z, G, cols), bf),
        vm((Z, G, cols), f32), vm((Z, G, cols), f32), vm((Z, 2 * T, cols), f32),
        vm((Z, T, cols), bf), vm((Z, T, cols), bf), vm((Z, T, cols), bf), vm((Z, T, cols), bf), vm((2 * T, cols), f32),
        dma((2,)), dma((C,)), dma((C,)), dma((C,)), dma((C,)), dma((V,)), dma((V,)), dma((Z,)), dma((Z,)),
        dma((Z,)), dma((Z,)), dma((Z, 2)), dma((Z, 2)),
        dma((2, Z)), dma((2, Z)), dma((2, Y, Z)), dma((2, Y, Z)), dma((2, Y, Z)), dma((2, Y, Z)), dma((Z,)), dma((Z,)),
        dma((Z, NU)), dma((Z, NU)), dma((far, NU)), dma((far, NU)), dma((NU,)), dma((NU,)),
        dma((2, Y)), dma((2, Y)), dma((2, Y1)), dma((2, Y1)), dma((1,)), dma((1,)), dma((Y,)), dma((Y,)),
        dma((Y1,)), dma((Y1,)),
        dma((Y,)), dma((Y,)), dma((Y1, Z)), dma((Y1, Z)), dma((Z,)), dma((Z,)), dma((Z,)), dma((Z,)),
    ]
    in_vmem = pl.BlockSpec(memory_space=pltpu.VMEM)
    anywhere = pl.BlockSpec(memory_space=pl.ANY)
    grad_hidden, prior_t, grad_embedding, slot_inputs, pre_grads = pl.pallas_call(
        functools.partial(kernel, (C, V, L, cap, top, K)),
        out_shape=(
            jax.ShapeDtypeStruct((T, cols), f32),
            jax.ShapeDtypeStruct((K, cols), f32),
            jax.ShapeDtypeStruct((D // C, words), bf),
            jax.ShapeDtypeStruct((L, D, Z * 2 * cap), bf),
            jax.ShapeDtypeStruct((Z, G, cols), bf),
        ),
        in_specs=[in_vmem] * 6 + [anywhere, anywhere],
        out_specs=(in_vmem,) * 5,
        scratch_shapes=scratch,
        compiler_params=pltpu.CompilerParams(
            collective_id=0, has_side_effects=True, vmem_limit_bytes=67043328
        ),
    )(
        hidden, routes.T, saved_lse.T, target_logprob.T, targets[None, :], prior_weight.T, projection, embedding
    )
    chunk = D // 4
    grad_hidden, prior_t, grad_embedding, grad_projection = pl.pallas_call(
        functools.partial(finish_kernel, (L, Z, cap, chunk)),
        out_shape=(
            jax.ShapeDtypeStruct((T, cols), f32),
            jax.ShapeDtypeStruct((K, cols), f32),
            jax.ShapeDtypeStruct((D // C, words), bf),
            jax.ShapeDtypeStruct((L, D, cols), bf),
        ),
        in_specs=[in_vmem] * 5,
        out_specs=(anywhere,) * 4,
        scratch_shapes=[vm((L, D, cols), bf), dma((3,)), dma((L, D // chunk))],
    )(grad_hidden, prior_t, grad_embedding, slot_inputs, pre_grads)
    return grad_hidden, prior_t.T, grad_projection, grad_embedding


def solution(mesh):
    owners, slices = mesh.shape["comp"], mesh.shape["vocab"]

    def body(hidden, routes, targets, saved_lse, target_logprob, prior_weight, projection, embedding):
        args = (hidden, routes, targets, saved_lse, target_logprob, prior_weight, projection, embedding)
        if fits(owners, slices, hidden, routes, projection, embedding):
            return fused(owners, slices, *args)
        return shards(*args)

    return jax.shard_map(
        body,
        mesh=mesh,
        in_specs=(
            P("comp", None),
            P("comp", None),
            P("comp"),
            P("comp", None),
            P("comp", None),
            P("vocab", None),
            P("comp", None, "vocab"),
            P(None, "vocab"),
        ),
        out_specs=(
            P("comp", "vocab"),
            P("vocab", None),
            P("comp", None, "vocab"),
            P("comp", "vocab"),
        ),
        check_vma=False,
    )
```

```python
import functools

import jax
import jax.numpy as jnp
from jax import lax
from jax.experimental import pallas as pl
from jax.experimental.pallas import tpu as pltpu
from jax.sharding import PartitionSpec as P

MESH = pl.DeviceIdType.MESH
HIGHEST = lax.Precision.HIGHEST
WORDS = 512


def core_swap(value, count):
    return lax.ppermute(value, "vocab", [(i, i ^ 1) for i in range(count)])


def vocab_gather(block, count):
    me = lax.axis_index("vocab")
    pairs = count // 2
    ring = [(i, (i + 2) % count) for i in range(count)]
    held = [block]
    for _ in range(pairs - 1):
        held.append(lax.ppermute(held[-1], "vocab", ring))
    own = jnp.stack(held)
    other = core_swap(own, count)
    core = me % 2
    both = jnp.where(core == 0, jnp.stack([own, other], 1), jnp.stack([other, own], 1))
    if pairs == 2:
        order = jnp.where(me // 2 == 0, both, both[::-1])
    else:
        order = jnp.take(both, (me // 2 - jnp.arange(pairs)) % pairs, axis=0)
    return order.reshape((count,) + block.shape)


def vocab_scatter(blocks, count, wire):
    me = lax.axis_index("vocab")
    pairs = count // 2
    core, row = me % 2, me // 2
    split = blocks.reshape((pairs, 2) + blocks.shape[1:])
    mine = jnp.where(core == 0, split[:, 0], split[:, 1])
    theirs = jnp.where(core == 0, split[:, 1], split[:, 0])
    mine = mine + core_swap(theirs.astype(wire), count).astype(jnp.float32)
    ring = [(i, (i + 2) % count) for i in range(count)]
    total = lax.dynamic_index_in_dim(mine, (row - 1) % pairs, 0, keepdims=False)
    for step in range(1, pairs):
        got = lax.ppermute(total.astype(wire), "vocab", ring).astype(jnp.float32)
        total = got + lax.dynamic_index_in_dim(mine, (row - 1 - step) % pairs, 0, keepdims=False)
    return total


def comp_scatter(z_rows, grad_rows, owners, wire):
    me = lax.axis_index("comp")
    order = list(range(0, owners, 2)) + list(range(1, owners, 2))[::-1]
    place_of = [order.index(i) for i in range(owners)]
    place = jnp.array(place_of, jnp.int32)[me]
    order_array = jnp.array(order, jnp.int32)
    rows = z_rows.shape[1] // owners
    half = rows // 2

    def part(sign, step):
        owner = order_array[(place - sign * (1 + step)) % owners]
        start = owner * rows + (0 if sign == 1 else half)
        block = lax.dynamic_slice_in_dim(z_rows, start, half, 1)
        return lax.dot_general(
            block, grad_rows, (((0,), (0,)), ((), ())), preferred_element_type=jnp.float32
        )

    totals = []
    rings = [
        (sign, [(order[p], order[(p + sign) % owners]) for p in range(owners)]) for sign in (1, -1)
    ]
    totals = [part(sign, 0) for sign, _ in rings]
    for step in range(1, owners):
        moved = [
            lax.ppermute(total.astype(wire), "comp", ring) for total, (_, ring) in zip(totals, rings)
        ]
        totals = [
            got.astype(jnp.float32) + part(sign, step) for got, (sign, _) in zip(moved, rings)
        ]
    return jnp.concatenate(totals, axis=0)


def shards(hidden, routes, targets, saved_lse, target_logprob, prior_weight, projection, embedding):
    highest = lax.Precision.HIGHEST
    tok_dev, model_width = hidden.shape
    top = routes.shape[1]
    comp_dev = projection.shape[0]
    cols = projection.shape[2]
    voc_dev = embedding.shape[1]
    owners = lax.axis_size("comp")
    slices = lax.axis_size("vocab")
    experts_all = comp_dev * owners
    capacity = max(2, (2 * tok_dev * top + experts_all - 1) // experts_all)
    slot_rows = owners * capacity
    comp_index = lax.axis_index("comp")
    vocab_index = lax.axis_index("vocab")
    wire = jnp.bfloat16 if owners <= 8 else jnp.float32

    own_cols = lax.dynamic_slice_in_dim(hidden, vocab_index * cols, cols, 1)
    cols_all = lax.all_gather(own_cols, "comp", axis=0, tiled=True)
    hidden_all = vocab_gather(cols_all, slices)

    partial_logits = jnp.dot(own_cols, prior_weight, preferred_element_type=jnp.float32)
    prior_logits = lax.psum(partial_logits, "vocab")
    comp_ids = jnp.arange(experts_all, dtype=jnp.int32)
    picked = (routes[:, :, None] == comp_ids[None, None, :]).astype(jnp.float32)
    selected = jnp.sum(picked * prior_logits[:, None, :], axis=2)
    gate = jax.nn.softmax(selected, axis=-1)
    posterior = jax.nn.softmax(jax.nn.log_softmax(selected, axis=-1) + target_logprob, axis=-1)
    prior_grads = jnp.sum((gate - posterior)[:, :, None] * picked, axis=1)
    prior_back = lax.dot_general(
        prior_grads, prior_weight.astype(jnp.float32), (((1,), (1,)), ((), ())), precision=highest
    )
    packed = jnp.concatenate(
        [
            posterior,
            saved_lse,
            jnp.repeat(targets.astype(jnp.float32)[:, None], top, axis=1),
            routes.astype(jnp.float32),
            prior_grads,
        ],
        axis=1,
    )
    packed_all = lax.all_gather(packed, "comp", axis=0, tiled=True)
    grad_prior = lax.dot_general(
        cols_all.astype(jnp.float32),
        packed_all[:, 4 * top :],
        (((0,), (0,)), ((), ())),
        precision=highest,
    )

    pairs = tok_dev * top

    def pair_values(index):
        return packed_all[:, index * top : (index + 1) * top].reshape(owners, pairs)

    pair_comp = pair_values(3)
    own_ids = (comp_index * comp_dev + jnp.arange(comp_dev, dtype=jnp.int32)).astype(jnp.float32)
    hit = pair_comp[None, :, :] == own_ids[:, None, None]
    pair_ids = jnp.arange(pairs, dtype=jnp.int32)
    before = (pair_ids[:, None] < pair_ids[None, :]).astype(jnp.bfloat16)
    rank = jnp.einsum(
        "lbp,pq->lbq", hit.astype(jnp.bfloat16), before, preferred_element_type=jnp.float32
    )
    place = jnp.where(hit, rank, -1.0)
    slot_ids = jnp.arange(capacity, dtype=jnp.int32).astype(jnp.float32)
    dispatch = (place[:, :, None, :] == slot_ids[None, None, :, None]).astype(jnp.float32)

    def to_slots(index):
        values = pair_values(index)
        return jnp.sum(dispatch * values[None, :, None, :], axis=3).reshape(comp_dev * slot_rows)

    post_rows, lse_rows = to_slots(0), to_slots(1)
    target_rows = to_slots(2).astype(jnp.int32)
    fold = (pair_ids[:, None] // top == jnp.arange(tok_dev, dtype=jnp.int32)[None, :]).astype(jnp.bfloat16)
    token_hit = jnp.einsum(
        "lbsp,pt->lbst", dispatch.astype(jnp.bfloat16), fold, preferred_element_type=jnp.float32
    ).astype(jnp.bfloat16)

    rows_in = jnp.einsum(
        "lbst,kbtd->lbskd",
        token_hit,
        hidden_all.reshape(slices, owners, tok_dev, cols),
        preferred_element_type=jnp.float32,
    ).astype(jnp.bfloat16).reshape(comp_dev, slot_rows, model_width)
    preact = jnp.einsum("lrd,lde->lre", rows_in, projection, preferred_element_type=jnp.float32)
    tanh_value = jnp.tanh(preact)
    z_local = tanh_value.astype(jnp.bfloat16).reshape(comp_dev * slot_rows, cols)
    z_blocks = vocab_gather(z_local, slices)
    z_all = jnp.swapaxes(z_blocks, 0, 1).reshape(comp_dev * slot_rows, slices * cols)
    logits = jnp.dot(z_all, embedding, preferred_element_type=jnp.float32)
    vocab_ids = vocab_index * voc_dev + jnp.arange(voc_dev, dtype=jnp.int32)
    target_hit = (target_rows[:, None] == vocab_ids[None, :]).astype(jnp.float32)
    logit_grads = (post_rows[:, None] * (jnp.exp(logits - lse_rows[:, None]) - target_hit)).astype(
        jnp.bfloat16
    )
    logit_grads = lax.optimization_barrier(logit_grads)
    feature_parts = jnp.einsum(
        "rv,kdv->krd",
        logit_grads,
        embedding.reshape(slices, cols, voc_dev),
        preferred_element_type=jnp.float32,
    )
    feature_grads = vocab_scatter(feature_parts, slices, wire).reshape(comp_dev, slot_rows, cols)
    pre_grads = (feature_grads * (1.0 - tanh_value * tanh_value)).astype(jnp.bfloat16)
    slot_parts = jnp.einsum(
        "lre,lkde->klrd",
        pre_grads,
        projection.reshape(comp_dev, slices, model_width // slices, cols),
        preferred_element_type=jnp.float32,
    )
    slot_share = vocab_scatter(slot_parts, slices, wire)
    token_parts = jnp.einsum(
        "lbst,lbsd->btd",
        token_hit.astype(jnp.float32),
        slot_share.reshape(comp_dev, owners, capacity, model_width // slices),
        precision=highest,
    )
    returned = lax.all_to_all(
        token_parts.astype(wire), "comp", split_axis=0, concat_axis=0, tiled=True
    )
    grad_hidden = jnp.sum(returned.astype(jnp.float32), axis=0) + prior_back
    grad_projection = jnp.einsum(
        "lrd,lre->lde", rows_in, pre_grads, preferred_element_type=jnp.float32
    ).astype(jnp.bfloat16)
    grad_embedding = comp_scatter(z_all, logit_grads, owners, wire).astype(jnp.bfloat16)
    return (grad_hidden, grad_prior, grad_projection, grad_embedding)


def capacity_of(owners, hidden, routes, projection):
    tok_dev, top = hidden.shape[0], routes.shape[1]
    experts_all = projection.shape[0] * owners
    return max(2, (2 * tok_dev * top + experts_all - 1) // experts_all)


def fits(owners, slices, hidden, routes, projection, embedding):
    capacity = capacity_of(owners, hidden, routes, projection)
    rows = hidden.shape[1] // owners
    return (
        owners // 2 == 4
        and slices % 2 == 0
        and capacity % 16 == 0
        and (2 * hidden.shape[0]) % 128 == 0
        and rows % 32 == 0
        and embedding.shape[1] % (2 * WORDS) == 0
        and projection.shape[2] % 128 == 0
    )


def nt_dot(a, b):
    return lax.dot_general(a, b, (((1,), (1,)), ((), ())), preferred_element_type=jnp.float32)


def kernel(
    dims,
    hidden_ref, routes_ref, lse_ref, tlp_ref, target_ref, pw_ref, proj_hbm, emb_hbm,
    gh_ref, gprior_ref, ge_ref, xt_hbm, pre_hbm,
    xt_ref, pre_ref, xs_ref, proj, emb, hid, infoa_out, infoa, places, infob_out, infob, pwall, dmat, cols3, tl, zall, zt, lg,
    xsend, xrecv, z1recv, z2recv, facc, fds, fdr, yas, yar, zas, zar,
    sds, sdr, sys, syr, ss, sacc, tokp, txs, txr, tzs, tzr, pback,
    load_sem, a_ss, a_rs, b_ss, b_rs, pw_ss, pw_rs, hz_ss, hz_rs, hx_ss, hx_rs, hd_ss, hd_rs,
    zd_ss, zd_rs, zy_ss, zy_rs, zf_ss, zf_rs, zz_ss, zz_rs, x_ss, x_rs, z1_ss, z1_rs, z2_ss, z2_rs,
    fd_ss, fd_rs, ya_ss, ya_rs, za_ss, za_rs,
    sd_ss, sd_rs, sy_ss, sy_rs, tx_ss, tx_rs, tz_ss, tz_rs,
):
    C, V, L, cap, top, K = dims
    Z, Y = C // 2, V // 2
    T, D = hidden_ref.shape
    cols = pw_ref.shape[1]
    W = emb_hbm.shape[1]
    WH = W // 2
    NJ = WH // WORDS
    NU = 2 * NJ
    G = L * 2 * cap
    S = Z * G
    half = D // 2
    R2 = D // C
    R = R2 // 2
    T2 = 2 * T
    bf, f32 = jnp.bfloat16, jnp.float32

    c, v = lax.axis_index("comp"), lax.axis_index("vocab")
    z, x = lax.div(c, 2), lax.rem(c, 2)
    y, k = lax.div(v, 2), lax.rem(v, 2)
    xo, ko = 1 - x, 1 - k
    partner = y * 2 + ko
    sw = lax.rem(z, 2)
    zp = z + 1 - 2 * sw
    pair = zp * 2 + x

    def zof(i):
        return lax.rem(z + i, Z)

    def zback(i):
        return lax.rem(z + Z - i, Z)

    def near_z(at, i):
        if Z != 4:
            return lax.rem(at + Z - i, Z)
        if i % 2:
            at = at + 1 - 2 * lax.rem(at, 2)
        if i // 2:
            at = at + 2 - 4 * lax.div(at, 2)
        return at

    def zto(i):
        return near_z(z, i) if Z == 4 else zof(i)

    def zfrom(i):
        return near_z(z, i)

    def yof(i):
        return lax.rem(y + i, Y)

    def yback(i):
        return lax.rem(y + Y - i, Y)

    def rcopy(src, dst, ss_, rs_, **dev):
        return pltpu.make_async_remote_copy(
            src_ref=src, dst_ref=dst, send_sem=ss_, recv_sem=rs_, device_id=dev, device_id_type=MESH
        )

    sends = []

    def send(copy):
        copy.start()
        sends.append(copy)

    load_p = pltpu.make_async_copy(proj_hbm, proj, load_sem.at[0])
    load_e = pltpu.make_async_copy(emb_hbm.at[:, pl.ds(pl.multiple_of(sw * WH, WH), WH)], emb, load_sem.at[1])
    load_p.start()
    load_e.start()

    comp_peers = [(i, r) for i in range(Z) for r in range(2) if (i, r) != (0, 0)]
    vocab_peers = [(i, r) for i in range(Y) for r in range(2) if (i, r) != (0, 0)]

    def comp_to(i, r):
        return zof(i) * 2 + lax.rem(x + r, 2)

    def comp_from(i, r):
        return zback(i) * 2 + lax.rem(x + r, 2)

    def vocab_to(i, r):
        return yof(i) * 2 + lax.rem(k + r, 2)

    def vocab_from(i, r):
        return yback(i) * 2 + lax.rem(k + r, 2)

    barrier = pltpu.get_barrier_semaphore()
    for dy in range(1, Y):
        pl.semaphore_signal(
            barrier, inc=1, device_id={"comp": pair, "vocab": yof(dy) * 2 + k}, device_id_type=MESH
        )
    for i, r in comp_peers:
        pl.semaphore_signal(barrier, inc=1, device_id={"comp": comp_to(i, r)}, device_id_type=MESH)
    for i, r in vocab_peers:
        pl.semaphore_signal(barrier, inc=1, device_id={"vocab": vocab_to(i, r)}, device_id_type=MESH)

    lane = lax.broadcasted_iota(jnp.int32, (K, T2), 1)
    mine = (lane >= x * T) & (lane < x * T + T)
    comp_id = lax.broadcasted_iota(jnp.int32, (K, T2), 0).astype(f32)
    hit = jnp.zeros((K, T2), f32)
    lse_k = jnp.zeros((K, T2), f32)
    tlp_k = jnp.zeros((K, T2), f32)

    def both(ref):
        value = ref[...].astype(f32)
        return jnp.concatenate([value, value], axis=1)

    route, lse_in, tlp_in, target_in = both(routes_ref), both(lse_ref), both(tlp_ref), both(target_ref)
    for j in range(top):
        named = (route[j : j + 1, :] == comp_id) & mine
        hit = jnp.where(named, 1.0, hit)
        lse_k = jnp.where(named, lse_in[j : j + 1, :], lse_k)
        tlp_k = jnp.where(named, tlp_in[j : j + 1, :], tlp_k)
    on = hit > 0.5
    upper = (
        lax.broadcasted_iota(jnp.int32, (T2, T2), 0) < lax.broadcasted_iota(jnp.int32, (T2, T2), 1)
    ).astype(f32).astype(bf)
    rank = jnp.dot(hit.astype(bf), upper, preferred_element_type=f32)
    place = jnp.where(on, rank, -1.0)
    infoa_out[...] = place.astype(bf)
    hid[z, pl.ds(pl.multiple_of(x * T, T), T), :] = hidden_ref[...]
    pwall[v] = pw_ref[...]
    pl.semaphore_wait(barrier, len(comp_peers) + len(vocab_peers) + Y - 1)

    xrow = pl.ds(pl.multiple_of(x * T, T), T)
    xorow = pl.ds(pl.multiple_of(xo * T, T), T)
    kcol = pl.ds(pl.multiple_of(k * half, half), half)
    kocol = pl.ds(pl.multiple_of(ko * half, half), half)
    for i, r in comp_peers:
        n = i * 2 + r
        send(rcopy(infoa_out, infoa.at[c], a_ss.at[n], a_rs.at[n], comp=comp_to(i, r)))
    send(rcopy(hidden_ref.at[:, kcol], hid.at[z, xrow, kcol], hx_ss.at[0], hx_rs.at[0], comp=z * 2 + xo))
    for i in range(1, Z):
        send(rcopy(hidden_ref.at[:, kcol], hid.at[z, xrow, kcol], hz_ss.at[i], hz_rs.at[i], comp=zto(i) * 2 + x))
    for i, r in vocab_peers:
        n = i * 2 + r
        send(rcopy(pw_ref, pwall.at[v], pw_ss.at[n], pw_rs.at[n], vocab=vocab_to(i, r)))
    infoa[c] = place.astype(bf)

    for i, r in vocab_peers:
        n = i * 2 + r
        rcopy(pw_ref, pwall.at[vocab_from(i, r)], pw_ss.at[n], pw_rs.at[n], vocab=vocab_from(i, r)).wait_recv()
    logit = jnp.zeros((K, T), f32)
    for vv in range(V):
        logit = logit + nt_dot(pwall[vv], hidden_ref[:, vv * cols : (vv + 1) * cols])
    logit = jnp.concatenate([logit, logit], axis=1)

    def top_of(values):
        return jnp.max(jnp.where(on, values, -1e30), axis=0, keepdims=True)

    def norm(values):
        total = jnp.sum(values, axis=0, keepdims=True)
        return jnp.where(total > 0.0, total, 1.0)

    shifted = logit - top_of(logit)
    weight = jnp.where(on, jnp.exp(jnp.where(on, shifted, 0.0)), 0.0)
    total = norm(weight)
    gate = weight / total
    mixed = shifted - jnp.log(total) + tlp_k
    mixed = jnp.where(on, mixed - top_of(mixed), 0.0)
    weight = jnp.where(on, jnp.exp(mixed), 0.0)
    post = weight / norm(weight)
    pgrad = gate - post
    target = jnp.where(mine[0:8], jnp.broadcast_to(target_in, (8, T2)), 0.0)
    infob_value = jnp.concatenate([post, lse_k, pgrad, target], axis=0)
    infob_out[...] = infob_value
    infob[c] = infob_value
    pback[...] = lax.dot_general(
        pgrad, pw_ref[...].astype(f32), (((0,), (0,)), ((), ())), precision=HIGHEST, preferred_element_type=f32
    )

    for i, r in comp_peers:
        n = i * 2 + r
        rcopy(infoa_out, infoa.at[comp_from(i, r)], a_ss.at[n], a_rs.at[n], comp=comp_from(i, r)).wait_recv()
    places[...] = infoa[...].astype(f32)
    slot_id = lax.broadcasted_iota(jnp.int32, (cap, T2), 0).astype(f32)
    for zz in range(Z):
        for l in range(L):
            for xx in range(2):
                row = places[zz * 2 + xx, pl.ds(c * L + l, 1), :]
                start = l * 2 * cap + xx * cap
                dmat[zz, start : start + cap, :] = (row == slot_id).astype(f32).astype(bf)

    def forward(i):
        if i > 0:
            rcopy(hidden_ref.at[:, kcol], hid.at[zfrom(i), xrow, kcol], hz_ss.at[i], hz_rs.at[i], comp=c).wait_recv()
            piece = hid.at[zfrom(i), xrow, kcol]
            send(rcopy(piece, piece, hx_ss.at[i], hx_rs.at[i], comp=z * 2 + xo))
            send(rcopy(piece, piece, hd_ss.at[i, 0], hd_rs.at[i, 0], vocab=partner))

    def forward_x(i):
        piece = hid.at[zfrom(i), xorow, kcol]
        rcopy(piece, piece, hx_ss.at[i], hx_rs.at[i], comp=z * 2 + xo).wait_recv()
        send(rcopy(piece, piece, hd_ss.at[i, 1], hd_rs.at[i, 1], vocab=partner))

    def arrive(i):
        if i > 0:
            piece = hid.at[zfrom(i), xrow, kocol]
            rcopy(piece, piece, hd_ss.at[i, 0], hd_rs.at[i, 0], vocab=partner).wait_recv()
        piece = hid.at[zfrom(i), xorow, kocol]
        rcopy(piece, piece, hd_ss.at[i, 1], hd_rs.at[i, 1], vocab=partner).wait_recv()

    def zpair(i):
        return near_z(zp, i)

    early_pair = max(0, Z - 3)

    def spread(side, i):
        piece = zall.at[side, v, zfrom(i) if side == 0 else zpair(i)]
        for dy in range(1, Y):
            if side == 0 or (early_pair <= i < Z - 1):
                send(rcopy(piece, piece, zy_ss.at[side, dy, i], zy_rs.at[side, dy, i], vocab=yof(dy) * 2 + k))
        send(rcopy(piece, piece, zd_ss.at[side, i], zd_rs.at[side, i], vocab=partner))

    def project(i):
        zz = zfrom(i)
        rows = jnp.dot(dmat[zz], hid[zz], preferred_element_type=f32).astype(bf)
        xs_ref[zz] = rows
        for l in range(L):
            span = slice(l * 2 * cap, (l + 1) * 2 * cap)
            value = jnp.tanh(jnp.dot(rows[span], proj[l], preferred_element_type=f32))
            tl[zz, span, :] = value
            zall[0, v, zz, span, :] = value.astype(bf)
        if i == Z - 1:
            for dy in range(1, Y):
                send(rcopy(
                    zall.at[0, v, zz], zall.at[1, v, zz], zy_ss.at[1, dy, i], zy_rs.at[1, dy, i],
                    comp=pair, vocab=yof(dy) * 2 + k,
                ))
        send(rcopy(zall.at[0, v, zz], zall.at[1, v, zz], zz_ss.at[i], zz_rs.at[i], comp=pair))
        spread(0, i)

    def relay(i):
        rcopy(zall.at[0, v, zpair(i)], zall.at[1, v, zpair(i)], zz_ss.at[i], zz_rs.at[i], comp=pair).wait_recv()
        spread(1, i)

    def cross(side, i):
        for dy in range(1, Y):
            piece = zall.at[side, yback(dy) * 2 + k, zfrom(i) if side == 0 else zpair(i)]
            rcopy(piece, piece, zy_ss.at[side, dy, i], zy_rs.at[side, dy, i], vocab=v).wait_recv()
            send(rcopy(piece, piece, zf_ss.at[side, dy, i], zf_rs.at[side, dy, i], vocab=partner))
            if side == 0 and i < early_pair:
                landing = zall.at[1, yback(dy) * 2 + k, zfrom(i)]
                send(rcopy(piece, landing, zy_ss.at[1, dy, i], zy_rs.at[1, dy, i], comp=pair))

    def zdone(side, i):
        piece = zall.at[side, partner, zfrom(i) if side == 0 else zpair(i)]
        rcopy(piece, piece, zd_ss.at[side, i], zd_rs.at[side, i], vocab=partner).wait_recv()

    def crossed(side, i):
        for dy in range(1, Y):
            piece = zall.at[side, yback(dy) * 2 + ko, zfrom(i) if side == 0 else zpair(i)]
            rcopy(piece, piece, zf_ss.at[side, dy, i], zf_rs.at[side, dy, i], vocab=partner).wait_recv()

    forward_x(0)
    if Z > 1:
        forward(1)
    load_p.wait()
    arrive(0)
    project(0)
    for i in range(1, Z):
        forward_x(i)
        if i + 1 < Z:
            forward(i + 1)
        arrive(i)
        project(i)
        if i == 1:
            for n_i, r in comp_peers:
                n = n_i * 2 + r
                send(rcopy(infob_out, infob.at[c], b_ss.at[n], b_rs.at[n], comp=comp_to(n_i, r)))
        relay(i - 1)
        if i > 1:
            cross(0, i - 2)

    for i, r in comp_peers:
        n = i * 2 + r
        rcopy(infob_out, infob.at[comp_from(i, r)], b_ss.at[n], b_rs.at[n], comp=comp_from(i, r)).wait_recv()
    for side in range(2):
        base = (c if side == 0 else pair) * L
        for zz in range(Z):
            for l in range(L):
                for xx in range(2):
                    b = zz * 2 + xx
                    start = l * 2 * cap + xx * cap
                    pick = places[b, pl.ds(base + l, 1), :] == slot_id
                    rows3 = (
                        infob[b, pl.ds(base + l, 1), :],
                        infob[b, pl.ds(K + base + l, 1), :],
                        infob[b, 3 * K : 3 * K + 1, :],
                    )
                    for q in range(3):
                        cols3[q, side, zz, start : start + cap, :] = jnp.sum(
                            jnp.where(pick, rows3[q], 0.0), axis=1, keepdims=True
                        )
    load_e.wait()

    def feature_rows(vv):
        return pl.ds(pl.multiple_of(vv * cols, cols), cols)

    def group_at(side, i):
        return zfrom(i) if side == 0 else zpair(i)

    def span_of(side, i):
        return pl.ds(pl.multiple_of(side * S + group_at(side, i) * G, G), G)

    def of_group(q, i):
        return jnp.concatenate([cols3[q, side, group_at(side, i)] for side in range(2)], axis=0)

    def logits_of(i):
        post_rows, lse_rows, target_rows = of_group(0, i), of_group(1, i), of_group(2, i).astype(jnp.int32)

        def words(j, carry):
            at = pl.ds(pl.multiple_of(j * WORDS, WORDS), WORDS)
            logits = jnp.zeros((2 * G, WORDS), f32)
            for vv in range(V):
                rows = jnp.concatenate([zall[side, vv, group_at(side, i)] for side in range(2)], axis=0)
                logits = logits + jnp.dot(rows, emb[vv * cols : (vv + 1) * cols, at], preferred_element_type=f32)
            ids = v * W + sw * WH + j * WORDS + lax.broadcasted_iota(jnp.int32, (2 * G, WORDS), 1)
            onehot = (target_rows == ids).astype(f32)
            value = (post_rows * (jnp.exp(logits - lse_rows) - onehot)).astype(bf)
            for side in range(2):
                lg[j, span_of(side, i), :] = value[side * G : (side + 1) * G]
            return carry

        lax.fori_loop(0, NJ, words, 0)

    def turn_group(i):
        for side in range(2):
            for vv in range(V):
                zt[vv * cols : (vv + 1) * cols, span_of(side, i)] = zall[side, vv, group_at(side, i)].T

    def complete(i):
        zdone(0, i)
        zdone(1, i)
        crossed(0, i)
        crossed(1, i)

    def finished(i):
        complete(i)
        turn_group(i)
        logits_of(i)

    cross(1, 0)
    cross(0, 2)
    finished(0)
    cross(1, 1)
    finished(1)
    relay(3)
    cross(0, 3)
    cross(1, 2)
    finished(2)
    cross(1, 3)
    finished(3)

    def owner_z(t):
        near = lax.rem(z + 2 * lax.rem(1 + lax.div(t, 2), Z // 2), Z)
        other = near + 1 - 2 * lax.rem(near, 2)
        e = 1 - lax.rem(t, 2)
        return e * other + (1 - e) * near

    def partial(xx, t, q):
        j, fh = lax.div(q, 2), lax.rem(q, 2)
        owner = owner_z(t) * 2 + xx
        rows = pl.ds(pl.multiple_of(owner * R2 + fh * R, R), R)
        return jnp.dot(zt[rows, :], lg[j], preferred_element_type=f32)

    def x_copy(t, q):
        return rcopy(xsend.at[t, q], xrecv.at[t, q], x_ss.at[t, q], x_rs.at[t, q], comp=z * 2 + xo)

    inner = lax.div(lax.rem(z + 1, Z), 2)

    def z1_copy(t, q):
        goal = lax.rem(z + 2 * (1 + lax.div(t, 2)), Z) * 2 + x
        return rcopy(xrecv.at[t, q], z1recv.at[t, q], z1_ss.at[t, q], z1_rs.at[t, q], comp=goal)

    def z2_copy(q):
        return rcopy(xrecv.at[Z - 2, q], z2recv.at[q], z2_ss.at[q], z2_rs.at[q], comp=pair)

    def xput(n, carry):
        t, q = lax.div(n, NU), lax.rem(n, NU)
        xsend[t, q] = partial(xo, t, q).astype(bf)
        x_copy(t, q).start()
        return carry

    def far_event(n, carry):
        t, q = lax.div(n, NU), lax.rem(n, NU)
        value = partial(x, t, q)
        x_copy(t, q).wait_recv()
        xrecv[t, q] = (value + xrecv[t, q].astype(f32)).astype(bf)
        z1_copy(t, q).start()
        return carry

    def near_value(te, q):
        t = Z - 2 + te
        value = partial(x, t, q)
        x_copy(t, q).wait_recv()
        value = value + xrecv[t, q].astype(f32)
        for dp in range(Z // 2 - 1):
            z1_copy(2 * dp + te, q).wait_recv()
            value = value + z1recv[2 * dp + te, q].astype(f32)
        return value.astype(bf)

    def near_event(q, carry):
        xrecv[Z - 2, q] = near_value(0, q)
        z2_copy(q).start()
        return carry

    def place_of(q, half):
        j, fh = lax.div(q, 2), lax.rem(q, 2)
        return (
            pl.ds(pl.multiple_of(fh * R, R), R),
            pl.ds(pl.multiple_of(half * WH + j * WORDS, WORDS), WORDS),
        )

    def own_event(q, carry):
        rows, at = place_of(q, sw)
        ge_ref[rows, at] = near_value(1, q)
        return carry

    def last_event(q, carry):
        z2_copy(q).wait_recv()
        rows, at = place_of(q, 1 - sw)
        ge_ref[rows, at] = z2recv[q]
        return carry

    events = {"x": [0, Z * NU, xput], "far": [0, (Z - 2) * NU, far_event], "near": [0, NU, near_event],
              "own": [0, NU, own_event], "last": [0, NU, last_event]}

    far_total = (Z - 2) * NU
    done = [0, 0]

    def run_far(outer_count, inner_count):
        for group, count in enumerate((outer_count, inner_count)):
            start, end = done[group], min(done[group] + count, far_total)
            done[group] = end
            if end > start:

                @pl.when(inner == group)
                def _():
                    lax.fori_loop(start, end, far_event, 0)

    def run(kind, count):
        entry = events[kind]
        end = min(entry[0] + count, entry[1])
        if end > entry[0]:
            lax.fori_loop(entry[0], end, entry[2], 0)
        entry[0] = end

    run("x", NU)

    def feature_part(side, vv):
        def add(j, total):
            at = pl.ds(pl.multiple_of(j * WORDS, WORDS), WORDS)
            return total + nt_dot(lg[j, side * S : (side + 1) * S, :], emb[feature_rows(vv), at])

        total = nt_dot(lg[0, side * S : (side + 1) * S, :], emb[feature_rows(vv), 0:WORDS])
        for j in range(1, NJ):
            total = add(j, total)
        return total

    def feature_swap(side, dy):
        return rcopy(fds.at[side, dy], fdr.at[side, dy], fd_ss.at[side, dy], fd_rs.at[side, dy], vocab=partner)

    def give(side, dy):
        fds[side, dy] = feature_part(side, yof(dy) * 2 + ko).astype(bf)
        send(feature_swap(side, dy))

    def take(side, dy):
        value = feature_part(side, yof(dy) * 2 + k)
        feature_swap(side, dy).wait_recv()
        facc[side, dy] = value + fdr[side, dy].astype(f32)

    H = S // 2

    def ya_copy(side, dy, n):
        return rcopy(
            yas.at[side, dy - 1, n], yar.at[side, dy - 1, n], ya_ss.at[side, dy - 1, n], ya_rs.at[side, dy - 1, n],
            vocab=yof(dy) * 2 + k,
        )

    def za_copy(n):
        return rcopy(zas.at[n], zar.at[n], za_ss.at[n], za_rs.at[n], comp=pair)

    def ya_out(side, dy):
        for n in range(2):
            yas[side, dy - 1, n] = facc[side, dy, n * H : (n + 1) * H, :].astype(bf)
            send(ya_copy(side, dy, n))

    def gathered(side, n):
        value = facc[side, 0, n * H : (n + 1) * H, :]
        for dy in range(1, Y):
            ya_copy(side, dy, n).wait_recv()
            value = value + yar[side, dy - 1, n].astype(f32)
        return value

    def za_out(n):
        zas[n] = gathered(1, n).astype(bf)
        send(za_copy(n))

    def pre_out(n):
        total = gathered(0, n)
        za_copy(n).wait_recv()
        total = total + zar[n].astype(f32)
        zspan = slice(n * Z // 2, (n + 1) * Z // 2)
        tanh_value = tl[zspan].reshape(H, cols)
        pre_ref[zspan] = (total * (1.0 - tanh_value * tanh_value)).astype(bf).reshape(Z // 2, G, cols)

    def turned(d, carry):
        at = pl.ds(pl.multiple_of(d * cols, cols), cols)
        for l in range(L):
            rows = xs_ref[:, l * 2 * cap : (l + 1) * 2 * cap, at].reshape(Z * 2 * cap, cols)
            xt_ref[l, at, :] = rows.T
        return carry

    def prior_out():
        owncols = pl.ds(pl.multiple_of(v * cols, cols), cols)
        gp = jnp.zeros((K, cols), f32)
        for zz in range(Z):
            grads = infob[zz * 2, 2 * K : 3 * K, :] + infob[zz * 2 + 1, 2 * K : 3 * K, :]
            gp = gp + jnp.dot(grads, hid[zz, :, owncols].astype(f32), precision=HIGHEST, preferred_element_type=f32)
        gprior_ref[...] = gp

    for dy in range(1, Y):
        give(1, dy)
        take(1, dy)
        ya_out(1, dy)
    for dy in range(1, Y):
        give(0, dy)
        run("x", 1)
        run_far(0, 1)
        take(0, dy)
        ya_out(0, dy)
    give(1, 0)
    run_far(0, 1)
    take(1, 0)
    run_far(0, 1)
    za_out(0)
    give(0, 0)
    run("x", 2)
    take(0, 0)
    run_far(1, 1)
    lax.fori_loop(0, V, turned, 0)
    store_xt = pltpu.make_async_copy(xt_ref, xt_hbm, load_sem.at[2])
    store_xt.start()
    za_out(1)
    run_far(4, 1)
    run("x", 2)
    prior_out()
    pre_out(0)
    run_far(1, 1)
    run("x", 2)
    run_far(1, 1)
    pre_out(1)
    store_pre = pltpu.make_async_copy(pre_ref, pre_hbm, load_sem.at[3])
    store_pre.start()

    def slot_part(vv):
        for l in range(L):
            span = slice(l * 2 * cap, (l + 1) * 2 * cap)
            rows = pre_ref[:, span, :].reshape(Z * 2 * cap, cols)
            ss[:, span, :] = nt_dot(rows, proj[l, feature_rows(vv), :]).reshape(Z, 2 * cap, cols)

    def slot_swap(dy):
        return rcopy(sds.at[dy], sdr.at[dy], sd_ss.at[dy], sd_rs.at[dy], vocab=partner)

    def sy_copy(dy, i):
        zz = zof(i)
        return rcopy(
            sys.at[dy - 1, zz], syr.at[dy - 1, zz], sy_ss.at[dy - 1, i], sy_rs.at[dy - 1, i], vocab=yof(dy) * 2 + k
        )

    order = list(range(1, Z)) + [0]
    for dy in range(1, Y):
        slot_part(yof(dy) * 2 + ko)
        sds[dy] = ss[...].astype(bf)
        send(slot_swap(dy))
        run_far(1, 1)
        run("x", 1)
        slot_part(yof(dy) * 2 + k)
        slot_swap(dy).wait_recv()
        for i in order:
            sys[dy - 1, zof(i)] = (ss[zof(i)] + sdr[dy, zof(i)].astype(f32)).astype(bf)
            send(sy_copy(dy, i))
    slot_part(partner)
    sds[0] = ss[...].astype(bf)
    send(slot_swap(0))
    slot_part(v)
    slot_swap(0).wait_recv()
    sacc[...] = ss[...] + sdr[0].astype(f32)
    run_far(far_total, far_total)

    def tx_copy(i):
        return rcopy(txs.at[i], txr.at[i], tx_ss.at[i], tx_rs.at[i], comp=z * 2 + xo)

    def tz_copy(i):
        return rcopy(tzs.at[i], tzr.at[i], tz_ss.at[i], tz_rs.at[i], comp=zof(i) * 2 + x)

    def fold(i):
        zz = zof(i)
        value = sacc[zz]
        for dy in range(1, Y):
            sy_copy(dy, i).wait_recv()
            value = value + syr[dy - 1, zz].astype(f32)
        tokp[i] = lax.dot_general(
            dmat[zz].astype(f32), value, (((0,), (0,)), ((), ())), precision=HIGHEST, preferred_element_type=f32
        )
        txs[i] = tokp[i, xorow, :].astype(bf)
        send(tx_copy(i))

    def homeward(i):
        tx_copy(i).wait_recv()
        value = tokp[i, xrow, :] + txr[i].astype(f32)
        if i > 0:
            tzs[i] = value.astype(bf)
            send(tz_copy(i))
        return value

    for n, i in enumerate(order):
        fold(i)
        run("x", 1 if n < 2 else 0)
        run("near", 1)
        if n > 0:
            homeward(order[n - 1])
    run("x", Z * NU)
    run("near", 2)
    home = homeward(order[-1]) + pback[xrow, :]
    run("near", NU)
    run("own", NU - 1)
    for i in range(1, Z):
        tz_copy(i).wait_recv()
        home = home + tzr[i].astype(f32)
    gh_ref[...] = home
    run("own", NU)
    run("last", NU)

    store_xt.wait()
    store_pre.wait()
    for copy in sends:
        copy.wait_send()

    def drain_x(n, carry):
        x_copy(lax.div(n, NU), lax.rem(n, NU)).wait_send()
        return carry

    def drain_z1(n, carry):
        z1_copy(lax.div(n, NU), lax.rem(n, NU)).wait_send()
        return carry

    def drain_z2(q, carry):
        z2_copy(q).wait_send()
        return carry

    lax.fori_loop(0, Z * NU, drain_x, 0)
    lax.fori_loop(0, (Z - 2) * NU, drain_z1, 0)
    lax.fori_loop(0, NU, drain_z2, 0)


def finish_kernel(dims, gh_ref, gprior_ref, ge_ref, xt_ref, pre_ref, gh_out, gprior_out, ge_out, out, buf, sem, out_sem):
    L, Z, cap, chunk = dims
    copies = [
        pltpu.make_async_copy(ge_ref, ge_out, sem.at[0]),
        pltpu.make_async_copy(gh_ref, gh_out, sem.at[1]),
        pltpu.make_async_copy(gprior_ref, gprior_out, sem.at[2]),
    ]
    for copy in copies:
        copy.start()
    cols = pre_ref.shape[-1]
    for l in range(L):
        rows = pre_ref[:, l * 2 * cap : (l + 1) * 2 * cap, :].reshape(Z * 2 * cap, cols)
        for n in range(xt_ref.shape[1] // chunk):
            at = pl.ds(n * chunk, chunk)
            buf[l, at, :] = jnp.dot(xt_ref[l, at, :], rows, preferred_element_type=jnp.float32).astype(buf.dtype)
            copy = pltpu.make_async_copy(buf.at[l, at, :], out.at[l, at, :], out_sem.at[l, n])
            copy.start()
            copies.append(copy)
    for copy in copies:
        copy.wait()


def fused(owners, slices, hidden, routes, targets, saved_lse, target_logprob, prior_weight, projection, embedding):
    tok_dev, width = hidden.shape
    top = routes.shape[1]
    comp_dev, _, cols = projection.shape
    words = embedding.shape[1]
    experts = comp_dev * owners
    cap = capacity_of(owners, hidden, routes, projection)
    C, V, L, T, K, D = owners, slices, comp_dev, tok_dev, experts, width
    Z, Y = C // 2, V // 2
    G, R = L * 2 * cap, D // C // 2
    bf, f32 = jnp.bfloat16, jnp.float32
    dma = pltpu.SemaphoreType.DMA
    vm = pltpu.VMEM
    rows_b = 3 * K + 8
    S, H, NJ = Z * G, Z * G // 2, words // 2 // WORDS
    NU, Y1, far = 2 * NJ, max(1, Y - 1), max(1, Z - 2)
    scratch = [
        vm((L, D, Z * 2 * cap), bf), vm((Z, G, cols), bf),
        vm((Z, G, D), bf), vm((L, D, cols), bf), vm((D, words // 2), bf), vm((Z, 2 * T, D), bf),
        vm((K, 2 * T), bf), vm((C, K, 2 * T), bf), vm((C, K, 2 * T), f32), vm((rows_b, 2 * T), f32), vm((C, rows_b, 2 * T), f32),
        vm((V, K, cols), bf), vm((Z, G, 2 * T), bf), vm((3, 2, Z, G, 1), f32), vm((Z, G, cols), f32),
        vm((2, V, Z, G, cols), bf), vm((D, 2 * S), bf), vm((NJ, 2 * S, WORDS), bf),
        vm((Z, NU, R, WORDS), bf), vm((Z, NU, R, WORDS), bf), vm((far, NU, R, WORDS), bf), vm((NU, R, WORDS), bf),
        vm((2, Y, S, cols), f32), vm((2, Y, S, cols), bf), vm((2, Y, S, cols), bf),
        vm((2, Y1, 2, H, cols), bf), vm((2, Y1, 2, H, cols), bf), vm((2, H, cols), bf), vm((2, H, cols), bf),
        vm((Y, Z, G, cols), bf), vm((Y, Z, G, cols), bf), vm((Y1, Z, G, cols), bf), vm((Y1, Z, G, cols), bf),
        vm((Z, G, cols), f32), vm((Z, G, cols), f32), vm((Z, 2 * T, cols), f32),
        vm((Z, T, cols), bf), vm((Z, T, cols), bf), vm((Z, T, cols), bf), vm((Z, T, cols), bf), vm((2 * T, cols), f32),
        dma((4,)), dma((C,)), dma((C,)), dma((C,)), dma((C,)), dma((V,)), dma((V,)), dma((Z,)), dma((Z,)),
        dma((Z,)), dma((Z,)), dma((Z, 2)), dma((Z, 2)),
        dma((2, Z)), dma((2, Z)), dma((2, Y, Z)), dma((2, Y, Z)), dma((2, Y, Z)), dma((2, Y, Z)), dma((Z,)), dma((Z,)),
        dma((Z, NU)), dma((Z, NU)), dma((far, NU)), dma((far, NU)), dma((NU,)), dma((NU,)),
        dma((2, Y)), dma((2, Y)), dma((2, Y1, 2)), dma((2, Y1, 2)), dma((2,)), dma((2,)),
        dma((Y,)), dma((Y,)), dma((Y1, Z)), dma((Y1, Z)), dma((Z,)), dma((Z,)), dma((Z,)), dma((Z,)),
    ]
    in_vmem = pl.BlockSpec(memory_space=pltpu.VMEM)
    anywhere = pl.BlockSpec(memory_space=pl.ANY)
    grad_hidden, prior_t, grad_embedding, slot_inputs, pre_grads = pl.pallas_call(
        functools.partial(kernel, (C, V, L, cap, top, K)),
        out_shape=(
            jax.ShapeDtypeStruct((T, cols), f32),
            jax.ShapeDtypeStruct((K, cols), f32),
            jax.ShapeDtypeStruct((D // C, words), bf),
            jax.ShapeDtypeStruct((L, D, Z * 2 * cap), bf),
            jax.ShapeDtypeStruct((Z, G, cols), bf),
        ),
        in_specs=[in_vmem] * 6 + [anywhere, anywhere],
        out_specs=(in_vmem,) * 3 + (anywhere,) * 2,
        scratch_shapes=scratch,
        compiler_params=pltpu.CompilerParams(
            collective_id=0, has_side_effects=True, vmem_limit_bytes=67043328
        ),
    )(
        hidden, routes.T, saved_lse.T, target_logprob.T, targets[None, :], prior_weight.T, projection, embedding
    )
    chunk = D // 4
    grad_hidden, prior_t, grad_embedding, grad_projection = pl.pallas_call(
        functools.partial(finish_kernel, (L, Z, cap, chunk)),
        out_shape=(
            jax.ShapeDtypeStruct((T, cols), f32),
            jax.ShapeDtypeStruct((K, cols), f32),
            jax.ShapeDtypeStruct((D // C, words), bf),
            jax.ShapeDtypeStruct((L, D, cols), bf),
        ),
        in_specs=[in_vmem] * 5,
        out_specs=(anywhere,) * 4,
        scratch_shapes=[vm((L, D, cols), bf), dma((3,)), dma((L, D // chunk))],
    )(grad_hidden, prior_t, grad_embedding, slot_inputs, pre_grads)
    return grad_hidden, prior_t.T, grad_projection, grad_embedding


def solution(mesh):
    owners, slices = mesh.shape["comp"], mesh.shape["vocab"]

    def body(hidden, routes, targets, saved_lse, target_logprob, prior_weight, projection, embedding):
        args = (hidden, routes, targets, saved_lse, target_logprob, prior_weight, projection, embedding)
        if fits(owners, slices, hidden, routes, projection, embedding):
            return fused(owners, slices, *args)
        return shards(*args)

    return jax.shard_map(
        body,
        mesh=mesh,
        in_specs=(
            P("comp", None),
            P("comp", None),
            P("comp"),
            P("comp", None),
            P("comp", None),
            P("vocab", None),
            P("comp", None, "vocab"),
            P(None, "vocab"),
        ),
        out_specs=(
            P("comp", "vocab"),
            P("vocab", None),
            P("comp", None, "vocab"),
            P("comp", "vocab"),
        ),
        check_vma=False,
    )
```
